256 devices in a mesh: lon: 16 (over y_hi, z), day: 16 (over x, y_lo, core).
Axes of the slice: x: 4, y: 4 (y_hi: 2, y_lo: 2; y = y_hi * 2 + y_lo), z: 8, core: 2. Of those that a mesh axis runs over, the one named last changes fastest.
Arguments:
- field: bfloat16 [368, 1440, 1024], P('day', 'lon'), may hold values from -6 to 6
Outputs:
- filtered: float32 [368, 1440, 1024], P('day', 'lon')
The draws below stay inside these ranges and needn't reach their ends.
All inputs are finite; a program needn't handle non-finite values.
Results may differ from the reference program's by a relative error of at most 0.0003.
Values may be sent and summed in bfloat16 or wider, within the bound.
A program may use at most 192 MiB of HBM per device.

```python
import jax
import jax.numpy as jnp
from jax import lax

COLS = 1024
LON = 1440
DAYS = 368
DAY_HALF = 15
LON_HALF = 10


def levels(stream_key, extent, cuts, least, top_value):
    def one(position, shards_of):
        draws = jax.random.uniform(jax.random.fold_in(jax.random.fold_in(stream_key, 6), position), (shards_of,), jnp.float32, least / len(cuts), top_value / len(cuts))
        return jnp.repeat(jnp.exp(draws), extent[position] // shards_of).reshape((-1,) + (1,) * (len(extent) - position - 1))

    level = one(*cuts[0])
    for cut in cuts[1:]:
        level = level * one(*cut)
    return level


def centred(stream_key, dims, deviation, reach, shards=(), kind=jnp.bfloat16):
    drawn = jax.random.normal(stream_key, dims, jnp.float32) * deviation
    if len(shards) > 0:
        drawn = levels(stream_key, dims, shards, -0.22, 0.18) * drawn
    return jnp.clip(drawn, min=-reach, max=reach).astype(kind)


def setup_inputs(seed: int = 0) -> dict:
    key_list = jax.random.split(jax.random.key(seed), 2)
    field = centred(key_list[0], (DAYS, LON, COLS), 1.0, 6.0, ((0, 16), (1, 16)))
    return {"field": field}


def running(values, dim, half):
    count = values.shape[dim] - 2 * half
    total = jnp.cumsum(values, axis=dim)
    first = jnp.zeros_like(lax.slice_in_dim(total, 0, 1, axis=dim))
    total = jnp.concatenate([first, total], axis=dim)
    upper = lax.slice_in_dim(total, 2 * half + 1, 2 * half + 1 + count, axis=dim)
    lower = lax.slice_in_dim(total, 0, count, axis=dim)
    return (upper - lower) / (2.0 * half + 1.0)


def wrapped(values, dim, half):
    size = values.shape[dim]
    head = lax.slice_in_dim(values, size - half, size, axis=dim)
    tail = lax.slice_in_dim(values, 0, half, axis=dim)
    return jnp.concatenate([head, values, tail], axis=dim)


def one_block(block):
    values = block.astype(jnp.float32)
    clim = running(wrapped(values, 0, DAY_HALF), 0, DAY_HALF)
    anomaly = values - clim
    return running(wrapped(anomaly, 1, LON_HALF), 1, LON_HALF)


def reference(field):
    width = 128 if COLS % 128 == 0 else COLS
    blocks = COLS // width
    split = field.reshape(DAYS, LON, blocks, width)
    split = jnp.moveaxis(split, 2, 0)
    result = lax.map(one_block, split)
    return jnp.moveaxis(result, 0, 2).reshape(DAYS, LON, COLS)
```

```python
import functools

import jax
import jax.numpy as jnp
import numpy as np
from jax import lax
from jax.experimental import pallas as pl
from jax.experimental.pallas import tpu as pltpu
from jax.sharding import PartitionSpec as P

DAY_HALF = 15
LON_HALF = 10
PLANES = 8
STEP = 10
TILE = 8
MESH = pl.DeviceIdType.MESH


def kernel(lons, days, field, tail, weights, out, own, near, far, terms, done, local_sem, send, recv, out_sem):
    count = field.shape[0]
    here = lax.axis_index("lon")
    day = lax.axis_index("day")
    core = lax.rem(day, 2)
    turn = 2 * core - 1
    far_day = lax.rem(day + turn + days, days)
    near_day = lax.rem(day - turn + days, days)
    east = lax.rem(here + 1, lons)
    west = lax.rem(here + lons - 1, lons)
    plane = lax.rem(here, PLANES)
    edge = LON_HALF
    wide = count + 2 * edge

    rows = pl.ds(pl.multiple_of(TILE * core, TILE), TILE)
    head_rows, tail_rows = pl.ds(0, TILE), pl.ds(TILE, TILE)

    partners = ((here, far_day), (here, near_day), (east, day), (west, day), (east, far_day), (west, far_day))
    barrier = pltpu.get_barrier_semaphore()
    for partner in partners:
        pl.semaphore_signal(barrier, inc=1, device_id=partner, device_id_type=MESH)
    load = pltpu.make_async_copy(field, own.at[pl.ds(edge, count)], local_sem)
    load.start()
    pl.semaphore_wait(barrier, len(partners))

    def remote(source, target, slot, device):
        return pltpu.make_async_remote_copy(
            src_ref=source, dst_ref=target, send_sem=send.at[slot], recv_sem=recv.at[slot],
            device_id=device, device_id_type=MESH,
        )

    chunks = (count - 2 * edge) // STEP
    low, high = pl.ds(0, edge), pl.ds(count - edge, edge)
    first, last = pl.ds(edge, edge), pl.ds(count, edge)
    before, after = pl.ds(0, edge), pl.ds(count + edge, edge)

    def pair(lon_span, target_span, slot, device):
        return (
            remote(field.at[lon_span, rows], far.at[target_span, head_rows], slot, device),
            remote(tail.at[lon_span], far.at[target_span, tail_rows], slot + 1, device),
        )

    to_east = remote(field.at[high], own.at[before], 0, (east, day))
    to_west = remote(field.at[low], own.at[after], 1, (west, day))
    far_edges = pair(low, first, 2, (here, far_day)) + pair(high, last, 4, (here, far_day))
    near_all = remote(field, near.at[pl.ds(edge, count)], 6, (here, near_day))
    near_before = remote(own.at[before], near.at[before], 7, (here, near_day))
    near_after = remote(own.at[after], near.at[after], 8, (here, near_day))
    east_direct = pair(high, before, 9, (east, far_day))
    west_direct = pair(low, after, 11, (west, far_day))
    east_relay = tuple(
        remote(far.at[last, part], far.at[before, part], 9 + i, (east, day)) for i, part in enumerate((head_rows, tail_rows))
    )
    west_relay = tuple(
        remote(far.at[first, part], far.at[after, part], 11 + i, (west, day)) for i, part in enumerate((head_rows, tail_rows))
    )
    bulk = [
        pair(pl.ds(edge + STEP * k, STEP), pl.ds(2 * edge + STEP * k, STEP), 13 + 2 * k, (here, far_day))
        for k in range(chunks)
    ]

    def start(copies):
        for copy in copies:
            copy.start()

    def arrive(copies):
        for copy in copies:
            copy.wait_recv()

    start((*far_edges, to_east, to_west))

    @pl.when(plane == PLANES - 1)
    def _():
        start(east_direct)

    @pl.when(plane == 0)
    def _():
        start(west_direct)

    near_all.start()
    for chunk in bulk:
        start(chunk)

    arrive((to_east, to_west))
    start((near_before, near_after))
    arrive(far_edges)

    @pl.when(plane != PLANES - 1)
    def _():
        start(east_relay)

    @pl.when(plane != 0)
    def _():
        start(west_relay)

    load.wait()
    near_all.wait_recv()

    def term(lon, _):
        total = jnp.dot(weights[core, 0], own[lon], preferred_element_type=jnp.float32)
        total += jnp.dot(weights[core, 1], near[lon], preferred_element_type=jnp.float32)
        total += jnp.dot(weights[core, 2, :, 0 : 2 * TILE], far[lon], preferred_element_type=jnp.float32)
        terms[lon] = total
        return _

    scale = 1.0 / ((2 * DAY_HALF + 1) * (2 * LON_HALF + 1))

    def result(lon, total):
        total = total + terms[lon + 2 * edge]
        done[lon] = total * scale
        return total - terms[lon]

    def put(start, size):
        return pltpu.make_async_copy(done.at[pl.ds(start, size)], out.at[pl.ds(start, size)], out_sem)

    arrive((near_before, near_after, *east_relay, *west_relay))
    lax.fori_loop(0, 2 * edge, term, 0)
    lax.fori_loop(count, wide, term, 0)
    total = lax.fori_loop(0, 2 * edge, lambda lon, total: total + terms[lon], jnp.zeros(terms.shape[1:], jnp.float32))
    for k in range(chunks):
        arrive(bulk[k])
        lax.fori_loop(2 * edge + STEP * k, 2 * edge + STEP * (k + 1), term, 0)
        total = lax.fori_loop(STEP * k, STEP * (k + 1), result, total)
        put(STEP * k, STEP).start()
    total = lax.fori_loop(STEP * chunks, count, result, total)
    put(STEP * chunks, count - STEP * chunks).start()

    sent = [to_east, to_west, *far_edges, near_all, near_before, near_after, *east_relay, *west_relay]
    for chunk in bulk:
        sent += chunk
    for copy in sent:
        copy.wait_send()
    put(0, count).wait()


def day_weights(rows):
    width = 2 * DAY_HALF + 1
    span = np.arange(-DAY_HALF, rows + DAY_HALF)
    window = np.abs(span[None, :] - np.arange(rows)[:, None]) <= DAY_HALF
    full = width * (span[None, :] == np.arange(rows)[:, None]) - 1.0 * window
    earlier, middle, later = full[:, :DAY_HALF], full[:, DAY_HALF : DAY_HALF + rows], full[:, DAY_HALF + rows :]
    table = np.zeros((2, 3, rows, rows), np.float32)
    table[:, 0] = middle
    table[0, 1, :, :DAY_HALF] = later
    table[1, 1, :, rows - DAY_HALF :] = earlier
    table[0, 2, :, :TILE] = earlier[:, :TILE]
    table[0, 2, :, TILE + 1 : 2 * TILE] = earlier[:, TILE:]
    table[1, 2, :, :DAY_HALF] = later
    return jnp.asarray(table, jnp.bfloat16)


def solution(mesh):
    lons, days = mesh.shape["lon"], mesh.shape["day"]

    def local(field):
        rows, count, columns = field.shape
        wide = count + 2 * LON_HALF
        slots = 13 + 2 * ((count - 2 * LON_HALF) // STEP)
        turned = jnp.transpose(field, (1, 0, 2))
        core = lax.rem(lax.axis_index("day"), 2)
        tail = jnp.where(core == 0, turned[:, TILE : 2 * TILE], turned[:, rows - TILE :])
        result = pl.pallas_call(
            functools.partial(kernel, lons, days),
            out_shape=jax.ShapeDtypeStruct((count, rows, columns), jnp.float32),
            in_specs=[pl.BlockSpec(memory_space=pl.ANY), pl.BlockSpec(memory_space=pl.ANY), pl.BlockSpec(memory_space=pltpu.VMEM)],
            out_specs=pl.BlockSpec(memory_space=pl.ANY),
            scratch_shapes=[
                pltpu.VMEM((wide, rows, columns), jnp.bfloat16),
                pltpu.VMEM((wide, rows, columns), jnp.bfloat16),
                pltpu.VMEM((wide, 2 * TILE, columns), jnp.bfloat16),
                pltpu.VMEM((wide, rows, columns), jnp.float32),
                pltpu.VMEM((count, rows, columns), jnp.float32),
                pltpu.SemaphoreType.DMA,
                pltpu.SemaphoreType.DMA((slots,)),
                pltpu.SemaphoreType.DMA((slots,)),
                pltpu.SemaphoreType.DMA,
            ],
            compiler_params=pltpu.CompilerParams(
                collective_id=0, has_side_effects=True, vmem_limit_bytes=60 * 1024 * 1024
            ),
            name="anomaly",
        )(turned, tail, day_weights(rows))
        return jnp.transpose(result, (1, 0, 2))

    return jax.shard_map(
        local, mesh=mesh, in_specs=(P("day", "lon", None),), out_specs=P("day", "lon", None), check_vma=False
    )
```

```python
import functools

import jax
import jax.numpy as jnp
import numpy as np
from jax import lax
from jax.experimental import pallas as pl
from jax.experimental.pallas import tpu as pltpu
from jax.sharding import PartitionSpec as P

DAY_HALF = 15
LON_HALF = 10
PLANES = 8
TILE = 8
REST = DAY_HALF - TILE
STEP = LON_HALF
PACKED = (STEP - 1) * TILE
MESH = pl.DeviceIdType.MESH


def kernel(lons, days, field, weights, out, own, near, heads, tails, packed, terms, local_sem, send, recv):
    count = field.shape[0]
    columns = field.shape[2]
    groups = count // STEP
    here = lax.axis_index("lon")
    day = lax.axis_index("day")
    core = lax.rem(day, 2)
    turn = 2 * core - 1
    far_day = lax.rem(day + turn + days, days)
    near_day = lax.rem(day - turn + days, days)
    east = lax.rem(here + 1, lons)
    west = lax.rem(here + lons - 1, lons)
    plane = lax.rem(here, PLANES)

    partners = ((here, far_day), (here, near_day), (east, day), (west, day), (east, far_day), (west, far_day))
    barrier = pltpu.get_barrier_semaphore()
    for partner in partners:
        pl.semaphore_signal(barrier, inc=1, device_id=partner, device_id_type=MESH)
    load = pltpu.make_async_copy(field, own.at[pl.ds(STEP, count)], local_sem)
    load.start()
    pl.semaphore_wait(barrier, len(partners))

    def remote(source, target, slot, device):
        return pltpu.make_async_remote_copy(
            src_ref=source, dst_ref=target, send_sem=send.at[slot], recv_sem=recv.at[slot],
            device_id=device, device_id_type=MESH,
        )

    def start(*copies):
        for copy in copies:
            copy.start()

    def arrive(*copies):
        for copy in copies:
            copy.wait_recv()

    def span(group):
        return pl.ds(STEP * group, STEP)

    head_rows = pl.ds(pl.multiple_of(TILE * core, TILE), TILE)
    final = groups - 1

    to_east = remote(field.at[span(final)], own.at[span(0)], 0, (east, day))
    to_west = remote(field.at[span(0)], own.at[span(groups + 1)], 1, (west, day))
    near_all = remote(field, near.at[pl.ds(STEP, count)], 2, (here, near_day))
    near_west = remote(own.at[span(0)], near.at[span(0)], 3, (here, near_day))
    near_east = remote(own.at[span(groups + 1)], near.at[span(groups + 1)], 4, (here, near_day))
    east_head_direct = remote(field.at[span(final), head_rows], heads.at[span(0)], 5, (east, far_day))
    west_head_direct = remote(field.at[span(0), head_rows], heads.at[span(groups + 1)], 6, (west, far_day))
    east_tail_direct = remote(packed.at[final], tails.at[0], 7, (east, far_day))
    west_tail_direct = remote(packed.at[0], tails.at[groups + 1], 8, (west, far_day))
    east_head = remote(heads.at[span(groups)], heads.at[span(0)], 5, (east, day))
    west_head = remote(heads.at[span(1)], heads.at[span(groups + 1)], 6, (west, day))
    east_tail = remote(tails.at[groups], tails.at[0], 7, (east, day))
    west_tail = remote(tails.at[1], tails.at[groups + 1], 8, (west, day))
    far_head = [
        remote(field.at[span(g), head_rows], heads.at[span(g + 1)], 9 + g, (here, far_day)) for g in range(groups)
    ]
    far_tail = [remote(packed.at[g], tails.at[g + 1], 9 + groups + g, (here, far_day)) for g in range(groups)]

    start(far_head[0], far_head[final], to_east, to_west)

    @pl.when(plane == PLANES - 1)
    def _():
        start(east_head_direct)

    @pl.when(plane == 0)
    def _():
        start(west_head_direct)

    start(near_all)
    load.wait()

    def rest(lon):
        rows = pl.ds(pl.multiple_of(TILE + TILE * core, TILE), REST)
        return own[lon, rows, :].astype(jnp.float32)

    def pack(group, _):
        base = STEP * (group + 1)
        spare = rest(base + STEP - 1)
        for j in range(STEP - 1):
            extra = spare[j % REST : j % REST + 1]
            tile = jnp.concatenate([rest(base + j), extra], axis=0)
            packed[group, TILE * j : TILE * (j + 1), :] = tile.astype(jnp.bfloat16)
        return _

    lax.fori_loop(0, groups, pack, 0)

    arrive(to_east, to_west)
    start(near_west, near_east, far_tail[0], far_tail[final])

    @pl.when(plane == PLANES - 1)
    def _():
        start(east_tail_direct)

    @pl.when(plane == 0)
    def _():
        start(west_tail_direct)

    for g in range(1, final):
        start(far_head[g], far_tail[g])

    arrive(far_head[0], far_head[final], far_tail[0], far_tail[final])

    @pl.when(plane != PLANES - 1)
    def _():
        start(east_head, east_tail)

    @pl.when(plane != 0)
    def _():
        start(west_head, west_tail)

    def term(group, _):
        base = STEP * group
        for j in range(STEP):
            lon = base + j
            total = jnp.dot(weights[core, 0, :, 0 : own.shape[1]], own[lon], preferred_element_type=jnp.float32)
            total += jnp.dot(weights[core, 1, :, 0 : own.shape[1]], near[lon], preferred_element_type=jnp.float32)
            total += jnp.dot(weights[core, 2, :, 0:TILE], heads[lon], preferred_element_type=jnp.float32)
            if j < STEP - 1:
                tile = tails[group, TILE * j : TILE * (j + 1), :]
                total += jnp.dot(weights[core, 3, :, 0:TILE], tile, preferred_element_type=jnp.float32)
            else:
                total += jnp.dot(weights[core, 4], tails[group], preferred_element_type=jnp.float32)
            terms[lon] = total
        return _

    scale = 1.0 / ((2 * DAY_HALF + 1) * (2 * LON_HALF + 1))

    def result(lon, total):
        total = total + terms[lon + 2 * STEP]
        out[lon] = total * scale
        return total - terms[lon]

    def results(group, total):
        return lax.fori_loop(STEP * group, STEP * (group + 1), result, total)

    def opening(group):
        zero = jnp.zeros(terms.shape[1:], jnp.float32)
        return lax.fori_loop(STEP * group, STEP * (group + 2), lambda lon, total: total + terms[lon], zero)

    arrive(near_all)
    lax.fori_loop(0, 2, lambda i, c: term(1 + final * i, c), 0)
    arrive(far_head[1], far_tail[1])
    term(2, 0)
    total = opening(1)
    corner = final // 2 + 1
    for g in range(2, final):
        arrive(far_head[g], far_tail[g])
        term(g + 1, 0)
        total = results(g - 1, total)
        if g == corner:
            arrive(near_west, near_east, east_head, west_head, east_tail, west_tail)
            lax.fori_loop(0, 2, lambda i, c: term((groups + 1) * i, c), 0)
            results(0, opening(0))
    for g in range(final - 1, groups):
        total = results(g, total)

    for copy in (to_east, to_west, near_all, near_west, near_east, east_head, west_head, east_tail, west_tail):
        copy.wait_send()
    for copy in far_head + far_tail:
        copy.wait_send()


def day_weights(rows):
    width = 2 * DAY_HALF + 1
    span = np.arange(-DAY_HALF, rows + DAY_HALF)
    window = np.abs(span[None, :] - np.arange(rows)[:, None]) <= DAY_HALF
    full = width * (span[None, :] == np.arange(rows)[:, None]) - 1.0 * window
    earlier, middle, later = full[:, :DAY_HALF], full[:, DAY_HALF : DAY_HALF + rows], full[:, DAY_HALF + rows :]
    table = np.zeros((2, 5, rows, PACKED), np.float32)
    table[:, 0, :, :rows] = middle
    table[0, 1, :, :DAY_HALF] = later
    table[1, 1, :, rows - DAY_HALF : rows] = earlier
    for core, far in enumerate((earlier, later)):
        table[core, 2, :, :TILE] = far[:, :TILE]
        table[core, 3, :, :REST] = far[:, TILE:]
        for j in range(REST):
            table[core, 4, :, TILE * j + REST] = far[:, TILE + j]
    return jnp.asarray(table, jnp.bfloat16)


def solution(mesh):
    lons, days = mesh.shape["lon"], mesh.shape["day"]

    def local(field):
        rows, count, columns = field.shape
        groups = count // STEP
        wide = count + 2 * STEP
        slots = 9 + 2 * groups
        result = pl.pallas_call(
            functools.partial(kernel, lons, days),
            out_shape=pltpu.VMEM((count, rows, columns), jnp.float32),
            in_specs=[pl.BlockSpec(memory_space=pltpu.HBM), pl.BlockSpec(memory_space=pltpu.VMEM)],
            out_specs=pl.BlockSpec(memory_space=pltpu.VMEM),
            scratch_shapes=[
                pltpu.VMEM((wide, rows, columns), jnp.bfloat16),
                pltpu.VMEM((wide, rows, columns), jnp.bfloat16),
                pltpu.VMEM((wide, TILE, columns), jnp.bfloat16),
                pltpu.VMEM((groups + 2, PACKED, columns), jnp.bfloat16),
                pltpu.VMEM((groups, PACKED, columns), jnp.bfloat16),
                pltpu.VMEM((wide, rows, columns), jnp.float32),
                pltpu.SemaphoreType.DMA,
                pltpu.SemaphoreType.DMA((slots,)),
                pltpu.SemaphoreType.DMA((slots,)),
            ],
            compiler_params=pltpu.CompilerParams(
                collective_id=0, has_side_effects=True, vmem_limit_bytes=44 * 1024 * 1024
            ),
            name="anomaly",
        )(jnp.transpose(field, (1, 0, 2)), day_weights(rows))
        return jnp.transpose(result, (1, 0, 2))

    return jax.shard_map(
        local, mesh=mesh, in_specs=(P("day", "lon", None),), out_specs=P("day", "lon", None), check_vma=False
    )
```

```python
import functools

import jax
import jax.numpy as jnp
from jax import lax
from jax.experimental import pallas as pl
from jax.experimental.pallas import tpu as pltpu
from jax.sharding import PartitionSpec as P

DAY_HALF = 15
LON_HALF = 10
PLANES = 8
TILE = 8
REST = DAY_HALF - TILE
STEP = LON_HALF
PACKED = (STEP - 1) * TILE
RELAYS = 3
SHARE = 3
KEPT = STEP - RELAYS * SHARE
MESH = pl.DeviceIdType.MESH


def kernel(lons, days, field, out, own, near, heads, tails, packed, terms, weights, relayed, ready, local_sem, send, recv):
    count = field.shape[0]
    columns = field.shape[2]
    groups = count // STEP
    here = lax.axis_index("lon")
    day = lax.axis_index("day")
    core = lax.rem(day, 2)
    turn = 2 * core - 1
    far_day = lax.rem(day + turn + days, days)
    near_day = lax.rem(day - turn + days, days)
    east = lax.rem(here + 1, lons)
    west = lax.rem(here + lons - 1, lons)
    plane = lax.rem(here, PLANES)

    barrier = pltpu.get_barrier_semaphore()

    def level(offset):
        return lax.rem(here + offset + lons, lons)

    def greet(*partners):
        for partner in partners:
            pl.semaphore_signal(barrier, inc=1, device_id=partner, device_id_type=MESH)

    reach = range(1, RELAYS + 1)
    eastmost = plane == PLANES - 1

    def at(spot):
        return functools.partial(pl.when, plane == spot)

    greet((here, far_day), (here, near_day))
    pl.when(plane != PLANES - 1)(functools.partial(greet, (east, day)))
    at(0)()(
        functools.partial(
            greet, (west, day), (west, far_day), *[(level(k), day) for k in reach[1:]], *[(level(-k - 1), day) for k in reach]
        )
    )
    for k in reach:
        at(k)()(functools.partial(greet, (level(-k - 1), day)))
    for k in reach[1:]:
        at(PLANES - 1 - k)()(functools.partial(greet, (level(k), day)))
    load = pltpu.make_async_copy(field, own.at[pl.ds(STEP, count)], local_sem)
    load.start()
    waits = {0: 2, 1: 3, PLANES - 1: 4 + 2 * RELAYS}
    for spot in range(PLANES):
        at(spot)()(functools.partial(pl.semaphore_wait, barrier, waits.get(spot, 4)))

    def tell(slot, *partners):
        for partner in partners:
            pl.semaphore_signal(ready.at[slot], inc=1, device_id=partner, device_id_type=MESH)

    pl.when(plane != 0)(functools.partial(tell, 0, (west, day)))

    @pl.when(eastmost)
    def _():
        tell(1, (east, day))
        tell(2, (east, far_day))
        tell(3, *[(level(-k), day) for k in reach[1:]])

    for k in reach:
        at(PLANES - 1 - k)()(functools.partial(tell, 4, (level(k + 1), day)))

    def remote(source, target, slot, device, sent=None):
        return pltpu.make_async_remote_copy(
            src_ref=source, dst_ref=target, send_sem=send.at[slot if sent is None else sent], recv_sem=recv.at[slot],
            device_id=device, device_id_type=MESH,
        )

    def start(*copies):
        for copy in copies:
            copy.start()

    def arrive(*copies):
        for copy in copies:
            copy.wait_recv()

    def span(group):
        return pl.ds(STEP * group, STEP)

    head_rows = pl.ds(pl.multiple_of(TILE * core, TILE), TILE)
    final = groups - 1

    to_east = remote(field.at[span(final)], own.at[span(0)], 0, (east, day))
    to_west = remote(field.at[span(0)], own.at[span(groups + 1)], 1, (west, day))
    near_all = remote(field, near.at[pl.ds(STEP, count)], 2, (here, near_day))
    near_west = remote(own.at[span(0)], near.at[span(0)], 3, (here, near_day))
    near_east = remote(own.at[span(groups + 1)], near.at[span(groups + 1)], 4, (here, near_day))
    east_head_direct = remote(field.at[span(final), head_rows], heads.at[span(0)], 5, (east, far_day))
    west_head_direct = remote(field.at[span(0), head_rows], heads.at[span(groups + 1)], 6, (west, far_day))
    east_tail_direct = remote(packed.at[final], tails.at[0], 7, (east, far_day))
    west_tail_direct = remote(packed.at[0], tails.at[groups + 1], 8, (west, far_day))
    east_head = remote(heads.at[span(groups)], heads.at[span(0)], 5, (east, day))
    west_head = remote(heads.at[span(1)], heads.at[span(groups + 1)], 6, (west, day))
    east_tail = remote(tails.at[groups], tails.at[0], 7, (east, day))
    west_tail = remote(tails.at[1], tails.at[groups + 1], 8, (west, day))
    spot = 9 + 2 * groups
    cut = [pl.ds(KEPT + SHARE * (k - 1), SHARE) for k in reach]
    east_part = [remote(field.at[pl.ds(STEP * final, KEPT)], own.at[pl.ds(0, KEPT)], 0, (east, day))]
    east_part += [
        remote(field.at[pl.ds(STEP * final + cut[k - 1].start, SHARE)], relayed, spot, (level(k + 1), day), spot + k)
        for k in reach
    ]
    west_part = [remote(field.at[pl.ds(0, KEPT)], own.at[pl.ds(STEP * (groups + 1), KEPT)], 1, (west, day))]
    west_part += [remote(field.at[cut[k - 1]], relayed, spot, (level(-k - 1), day), spot + k) for k in reach]
    east_pass = [remote(relayed, own.at[cut[k - 1]], 0, (level(-k), day), spot) for k in reach]
    west_pass = [
        remote(relayed, own.at[pl.ds(STEP * (groups + 1) + cut[k - 1].start, SHARE)], 1, (level(k), day), spot)
        for k in reach
    ]

    def each_plane(eastward, westward, act):
        for k in reach:
            pl.when(plane == k)(functools.partial(act, eastward[k - 1]))
            pl.when(plane == PLANES - 1 - k)(functools.partial(act, westward[k - 1]))

    far_head = [
        remote(field.at[span(g), head_rows], heads.at[span(g + 1)], 9 + g, (here, far_day)) for g in range(groups)
    ]
    far_tail = [remote(packed.at[g], tails.at[g + 1], 9 + groups + g, (here, far_day)) for g in range(groups)]

    start(far_head[0], far_head[final])

    @pl.when(eastmost)
    def _():
        start(*reversed(east_part), east_head_direct)

    @pl.when(plane != 0)
    def _():
        start(to_west)

    start(near_all)
    load.wait()

    def rest(lon):
        rows = pl.ds(pl.multiple_of(TILE + TILE * core, TILE), REST)
        return own[lon, rows, :].astype(jnp.float32)

    def pack(group, _):
        base = STEP * (group + 1)
        spare = rest(base + STEP - 1)
        for j in range(STEP - 1):
            extra = spare[j % REST : j % REST + 1]
            tile = jnp.concatenate([rest(base + j), extra], axis=0)
            packed[group, TILE * j : TILE * (j + 1), :] = tile.astype(jnp.bfloat16)
        return _

    lax.fori_loop(0, groups, pack, 0)

    start(far_tail[0], far_tail[final])

    @pl.when(eastmost)
    def _():
        start(east_tail_direct)

    for g in range(1, final):
        start(far_head[g], far_tail[g])

    @pl.when(plane != PLANES - 1)
    def _():
        pl.semaphore_wait(ready.at[0], 1)
        start(to_east)

    @pl.when(plane == 0)
    def _():
        for slot, count_of in ((1, 1), (2, 1), (4, RELAYS)):
            pl.semaphore_wait(ready.at[slot], count_of)
        start(*reversed(west_part), west_head_direct, west_tail_direct)

    for k in reach[1:]:
        at(PLANES - 1 - k)()(functools.partial(pl.semaphore_wait, ready.at[3], 1))

    def forward(copy):
        arrive(east_part[1])
        start(copy)

    each_plane(east_pass, west_pass, forward)
    arrive(to_east, to_west)
    start(near_west, near_east)
    arrive(far_head[0], far_head[final], far_tail[0], far_tail[final])

    @pl.when(plane != PLANES - 1)
    def _():
        start(east_head, east_tail)

    @pl.when(plane != 0)
    def _():
        start(west_head, west_tail)

    day_of = lax.broadcasted_iota(jnp.int32, weights.shape[1:], 0)
    place = lax.broadcasted_iota(jnp.int32, weights.shape[1:], 1)

    def window(position, valid=True):
        inside = (jnp.abs(position - day_of) <= DAY_HALF) & valid
        return jnp.where(inside, -1.0, 0.0)

    block = own.shape[1]
    earlier, later = 1 - core, core
    weights[0] = (window(place) + jnp.where(place == day_of, 2.0 * DAY_HALF + 1.0, 0.0)).astype(jnp.bfloat16)
    weights[1] = window(place + block * (earlier - later)).astype(jnp.bfloat16)
    weights[2] = window(place - DAY_HALF * earlier + block * later).astype(jnp.bfloat16)
    weights[3] = window(place - REST * earlier + (block + TILE) * later, place < REST).astype(jnp.bfloat16)
    which = place // TILE
    stray = (place % TILE == REST) & (which < REST)
    weights[4] = window(which - REST * earlier + (block + TILE) * later, stray).astype(jnp.bfloat16)

    def term(group, _):
        base = STEP * group
        for j in range(STEP):
            lon = base + j
            total = jnp.dot(weights[0, :, 0 : own.shape[1]], own[lon], preferred_element_type=jnp.float32)
            total += jnp.dot(weights[1, :, 0 : own.shape[1]], near[lon], preferred_element_type=jnp.float32)
            total += jnp.dot(weights[2, :, 0:TILE], heads[lon], preferred_element_type=jnp.float32)
            if j < STEP - 1:
                tile = tails[group, TILE * j : TILE * (j + 1), :]
                total += jnp.dot(weights[3, :, 0:TILE], tile, preferred_element_type=jnp.float32)
            else:
                total += jnp.dot(weights[4], tails[group], preferred_element_type=jnp.float32)
            terms[lon] = total
        return _

    scale = 1.0 / ((2 * DAY_HALF + 1) * (2 * LON_HALF + 1))

    def result(lon, total):
        total = total + terms[lon + 2 * STEP]
        out[lon] = total * scale
        return total - terms[lon]

    def results(group, total):
        return lax.fori_loop(STEP * group, STEP * (group + 1), result, total)

    def opening(group):
        zero = jnp.zeros(terms.shape[1:], jnp.float32)
        return lax.fori_loop(STEP * group, STEP * (group + 2), lambda lon, total: total + terms[lon], zero)

    arrive(near_all)
    lax.fori_loop(0, 2, lambda i, c: term(1 + final * i, c), 0)
    arrive(far_head[1], far_tail[1])
    term(2, 0)
    total = opening(1)
    corner = final // 2 + 1
    for g in range(2, final):
        arrive(far_head[g], far_tail[g])
        term(g + 1, 0)
        total = results(g - 1, total)
        if g == corner:
            arrive(near_west, near_east, east_head, west_head, east_tail, west_tail)
            lax.fori_loop(0, 2, lambda i, c: term((groups + 1) * i, c), 0)
            results(0, opening(0))
    for g in range(final - 1, groups):
        total = results(g, total)

    def finish(*copies):
        for copy in copies:
            copy.wait_send()

    each_plane(east_pass, west_pass, finish)

    @pl.when(plane == PLANES - 1)
    def _():
        finish(*east_part)

    @pl.when(plane != PLANES - 1)
    def _():
        finish(to_east)

    @pl.when(plane == 0)
    def _():
        finish(*west_part)

    @pl.when(plane != 0)
    def _():
        finish(to_west)

    for copy in (near_all, near_west, near_east, east_head, west_head, east_tail, west_tail):
        copy.wait_send()
    for copy in far_head + far_tail:
        copy.wait_send()


def solution(mesh):
    lons, days = mesh.shape["lon"], mesh.shape["day"]

    def local(field):
        rows, count, columns = field.shape
        groups = count // STEP
        wide = count + 2 * STEP
        slots = 10 + 2 * groups + RELAYS
        result = pl.pallas_call(
            functools.partial(kernel, lons, days),
            out_shape=pltpu.VMEM((count, rows, columns), jnp.float32),
            in_specs=[pl.BlockSpec(memory_space=pltpu.HBM)],
            out_specs=pl.BlockSpec(memory_space=pltpu.VMEM),
            scratch_shapes=[
                pltpu.VMEM((wide, rows, columns), jnp.bfloat16),
                pltpu.VMEM((wide, rows, columns), jnp.bfloat16),
                pltpu.VMEM((wide, TILE, columns), jnp.bfloat16),
                pltpu.VMEM((groups + 2, PACKED, columns), jnp.bfloat16),
                pltpu.VMEM((groups, PACKED, columns), jnp.bfloat16),
                pltpu.VMEM((wide, rows, columns), jnp.float32),
                pltpu.VMEM((5, rows, PACKED), jnp.bfloat16),
                pltpu.VMEM((SHARE, rows, columns), jnp.bfloat16),
                pltpu.SemaphoreType.REGULAR((5,)),
                pltpu.SemaphoreType.DMA,
                pltpu.SemaphoreType.DMA((slots,)),
                pltpu.SemaphoreType.DMA((slots,)),
            ],
            compiler_params=pltpu.CompilerParams(
                collective_id=0, has_side_effects=True, vmem_limit_bytes=44 * 1024 * 1024
            ),
            name="anomaly",
        )(jnp.transpose(field, (1, 0, 2)))
        return jnp.transpose(result, (1, 0, 2))

    return jax.shard_map(
        local, mesh=mesh, in_specs=(P("day", "lon", None),), out_specs=P("day", "lon", None), check_vma=False
    )
```

```python
import functools

import jax
import jax.numpy as jnp
from jax import lax
from jax.experimental import pallas as pl
from jax.experimental.pallas import tpu as pltpu
from jax.sharding import PartitionSpec as P

DAY_HALF = 15
LON_HALF = 10
PLANES = 8
TILE = 8
REST = DAY_HALF - TILE
STEP = LON_HALF
PACKED = (STEP - 1) * TILE
RELAYS = 3
LATE = 3
SHARE = 3
KEPT = STEP - RELAYS * SHARE
MESH = pl.DeviceIdType.MESH


def results(terms, target, group, first, total):
    scale = 1.0 / ((2 * DAY_HALF + 1) * (2 * LON_HALF + 1))

    def result(lon, total):
        total = total + terms[lon + 2 * STEP]
        target[lon - STEP * first] = total * scale
        return total - terms[lon]

    return lax.fori_loop(STEP * group, STEP * (group + 1), result, total)


def opening(terms, group):
    zero = jnp.zeros(terms.shape[1:], jnp.float32)
    return lax.fori_loop(STEP * group, STEP * (group + 2), lambda lon, total: total + terms[lon], zero)


def finishing(done, terms, out, late, sems):
    early = done.shape[0] // STEP

    def put(source, group, first):
        return pltpu.make_async_copy(
            source.at[pl.ds(STEP * (group - first), STEP)], out.at[pl.ds(STEP * group, STEP)], sems.at[group]
        )

    copies = [put(done, group, 0) for group in range(early)]
    for copy in copies:
        copy.start()
    total = opening(terms, early)
    for group in range(early, early + LATE):
        total = results(terms, late, group, early, total)
        copies.append(put(late, group, early))
        copies[-1].start()
    for copy in copies:
        copy.wait()


def kernel(
    lons, days, field, done, terms, own, near, heads, tails, packed, weights, relayed, ready,
    apart, wrap_heads, wrap_tails, wrap_rests, side_heads, side_tails, side_rests, local_sem, send, recv,
):
    count = field.shape[0]
    columns = field.shape[2]
    groups = count // STEP
    here = lax.axis_index("lon")
    day = lax.axis_index("day")
    core = lax.rem(day, 2)
    turn = 2 * core - 1
    far_day = lax.rem(day + turn + days, days)
    near_day = lax.rem(day - turn + days, days)
    east = lax.rem(here + 1, lons)
    west = lax.rem(here + lons - 1, lons)
    plane = lax.rem(here, PLANES)

    barrier = pltpu.get_barrier_semaphore()

    def level(offset):
        return lax.rem(here + offset + lons, lons)

    def greet(*partners):
        for partner in partners:
            pl.semaphore_signal(barrier, inc=1, device_id=partner, device_id_type=MESH)

    reach = range(1, RELAYS + 1)
    eastmost = plane == PLANES - 1

    def at(spot):
        return functools.partial(pl.when, plane == spot)

    greet((here, far_day), (here, near_day))
    pl.when(plane != PLANES - 1)(functools.partial(greet, (east, day)))
    at(0)()(
        functools.partial(
            greet, (west, day), (west, far_day), *[(level(k), day) for k in reach[1:]], *[(level(-k - 1), day) for k in reach]
        )
    )
    for k in reach:
        at(k)()(functools.partial(greet, (level(-k - 1), day)))
    for k in reach[1:]:
        at(PLANES - 1 - k)()(functools.partial(greet, (level(k), day)))
    load = pltpu.make_async_copy(field, own.at[pl.ds(STEP, count)], local_sem)
    load.start()
    waits = {0: 2, 1: 3, PLANES - 1: 4 + 2 * RELAYS}
    for spot in range(PLANES):
        at(spot)()(functools.partial(pl.semaphore_wait, barrier, waits.get(spot, 4)))

    def tell(slot, *partners):
        for partner in partners:
            pl.semaphore_signal(ready.at[slot], inc=1, device_id=partner, device_id_type=MESH)

    pl.when(plane != 0)(functools.partial(tell, 0, (west, day)))

    @pl.when(eastmost)
    def _():
        tell(1, (east, day))
        tell(2, (east, far_day))
        tell(3, *[(level(-k), day) for k in reach[1:]])

    for k in reach:
        at(PLANES - 1 - k)()(functools.partial(tell, 4, (level(k + 1), day)))

    def remote(source, target, slot, device, sent=None):
        return pltpu.make_async_remote_copy(
            src_ref=source, dst_ref=target, send_sem=send.at[slot if sent is None else sent], recv_sem=recv.at[slot],
            device_id=device, device_id_type=MESH,
        )

    def start(*copies):
        for copy in copies:
            copy.start()

    def arrive(*copies):
        for copy in copies:
            copy.wait_recv()

    def span(group):
        return pl.ds(STEP * group, STEP)

    head_rows = pl.ds(pl.multiple_of(TILE * core, TILE), TILE)
    final = groups - 1

    to_east = remote(field.at[span(final)], own.at[span(0)], 0, (east, day))
    to_west = remote(field.at[span(0)], own.at[span(groups + 1)], 1, (west, day))
    near_all = remote(field, near.at[pl.ds(STEP, count)], 2, (here, near_day))
    near_west = remote(own.at[span(0)], near.at[span(0)], 3, (here, near_day))
    near_east = remote(own.at[span(groups + 1)], near.at[span(groups + 1)], 4, (here, near_day))
    east_head_direct = remote(field.at[span(final), head_rows], heads.at[span(0)], 5, (east, far_day))
    west_head_direct = remote(field.at[span(0), head_rows], heads.at[span(groups + 1)], 6, (west, far_day))
    east_tail_direct = remote(packed.at[final], tails.at[0], 7, (east, far_day))
    west_tail_direct = remote(packed.at[0], tails.at[groups + 1], 8, (west, far_day))
    east_head = remote(heads.at[span(groups)], heads.at[span(0)], 5, (east, day))
    west_head = remote(heads.at[span(1)], heads.at[span(groups + 1)], 6, (west, day))
    east_tail = remote(tails.at[groups], tails.at[0], 7, (east, day))
    west_tail = remote(tails.at[1], tails.at[groups + 1], 8, (west, day))
    spot = 9 + 2 * groups
    cut = [pl.ds(KEPT + SHARE * (k - 1), SHARE) for k in reach]
    kept = pl.ds(0, KEPT)

    turned = spot + RELAYS + 1
    east_part = [remote(apart.at[kept], wrap_rests.at[kept], turned, (east, day))]
    east_part += [remote(apart.at[cut[k - 1]], relayed, spot, (level(k + 1), day), spot + k) for k in reach]
    west_part = [remote(apart.at[kept], wrap_rests.at[kept], turned, (west, day))]
    west_part += [remote(apart.at[cut[k - 1]], relayed, spot, (level(-k - 1), day), spot + k) for k in reach]
    east_pass = [remote(relayed, wrap_rests.at[cut[k - 1]], turned, (level(-k), day), spot) for k in reach]
    west_pass = [remote(relayed, wrap_rests.at[cut[k - 1]], turned, (level(k), day), spot) for k in reach]
    wrap_rest = remote(apart, wrap_rests, turned, (east, day))
    east_wrap = (
        remote(heads.at[span(groups)], wrap_heads, turned + 1, (east, far_day)),
        remote(tails.at[groups], wrap_tails, turned + 2, (east, far_day)),
    )
    west_wrap = (
        remote(heads.at[span(1)], wrap_heads, turned + 1, (west, far_day)),
        remote(tails.at[1], wrap_tails, turned + 2, (west, far_day)),
    )
    sides = tuple(
        remote(source, target, turned + 3 + i, (here, near_day))
        for i, (source, target) in enumerate(((wrap_heads, side_heads), (wrap_tails, side_tails), (wrap_rests, side_rests)))
    )

    def each_plane(eastward, westward, act):
        for k in reach:
            pl.when(plane == k)(functools.partial(act, eastward[k - 1]))
            pl.when(plane == PLANES - 1 - k)(functools.partial(act, westward[k - 1]))

    far_head = [
        remote(field.at[span(g), head_rows], heads.at[span(g + 1)], 9 + g, (here, far_day)) for g in range(groups)
    ]
    far_tail = [remote(packed.at[g], tails.at[g + 1], 9 + groups + g, (here, far_day)) for g in range(groups)]

    start(far_head[0], far_head[final])

    @pl.when(eastmost)
    def _():
        start(east_head_direct)

    @pl.when(plane != 0)
    def _():
        start(to_west)

    start(near_all)
    load.wait()

    def rest(lon):
        rows = pl.ds(pl.multiple_of(TILE + TILE * core, TILE), REST)
        return own[lon, rows, :].astype(jnp.float32)

    def pack(group, _):
        base = STEP * (group + 1)
        spare = rest(base + STEP - 1)
        for j in range(STEP - 1):
            extra = spare[j % REST : j % REST + 1]
            tile = jnp.concatenate([rest(base + j), extra], axis=0)
            packed[group, TILE * j : TILE * (j + 1), :] = tile.astype(jnp.bfloat16)
        return _

    lax.fori_loop(0, groups, pack, 0)

    ends = (plane == 0) | eastmost
    wrapped = plane // (PLANES - 1)

    @pl.when(ends)
    def _():
        def part(j, _):
            lon = STEP + STEP * final * wrapped + j
            low = own[lon, 0:TILE, :].astype(jnp.float32)
            high = own[lon, TILE:, :].astype(jnp.float32)
            apart[j] = jnp.where(core == 0, high[REST:], low).astype(jnp.bfloat16)
            return _

        lax.fori_loop(0, STEP, part, 0)

    start(far_tail[0], far_tail[final])

    @pl.when(eastmost)
    def _():
        start(*east_part, east_tail_direct)

    for g in range(1, final):
        start(far_head[g], far_tail[g])

    @pl.when(plane != PLANES - 1)
    def _():
        pl.semaphore_wait(ready.at[0], 1)
        start(to_east)

    @pl.when(plane == 0)
    def _():
        for slot, count_of in ((1, 1), (2, 1), (4, RELAYS)):
            pl.semaphore_wait(ready.at[slot], count_of)
        start(*west_part, west_head_direct, west_tail_direct)

    for k in reach[1:]:
        at(PLANES - 1 - k)()(functools.partial(pl.semaphore_wait, ready.at[3], 1))

    def forward(copy):
        arrive(east_part[1])
        start(copy)

    each_plane(east_pass, west_pass, forward)

    @pl.when(plane != 0)
    def _():
        arrive(to_east)
        start(near_west)

    @pl.when(plane != PLANES - 1)
    def _():
        arrive(to_west)
        start(near_east)

    arrive(far_head[0], far_head[final], far_tail[0], far_tail[final])

    @pl.when(plane != PLANES - 1)
    def _():
        start(east_head, east_tail)

    @pl.when(plane != 0)
    def _():
        start(west_head, west_tail)

    @pl.when(eastmost)
    def _():
        start(*east_wrap)

    @pl.when(plane == 0)
    def _():
        start(*west_wrap)

    @pl.when(ends)
    def _():
        arrive(wrap_rest, *east_wrap)
        start(*sides)

    day_of = lax.broadcasted_iota(jnp.int32, weights.shape[1:], 0)
    place = lax.broadcasted_iota(jnp.int32, weights.shape[1:], 1)

    def window(position, valid=True):
        inside = (jnp.abs(position - day_of) <= DAY_HALF) & valid
        return jnp.where(inside, -1.0, 0.0)

    block = own.shape[1]
    earlier, later = 1 - core, core
    weights[0] = (window(place) + jnp.where(place == day_of, 2.0 * DAY_HALF + 1.0, 0.0)).astype(jnp.bfloat16)
    weights[1] = window(place + block * (earlier - later)).astype(jnp.bfloat16)
    weights[2] = window(place - DAY_HALF * earlier + block * later).astype(jnp.bfloat16)
    weights[3] = window(place - REST * earlier + (block + TILE) * later, place < REST).astype(jnp.bfloat16)
    which = place // TILE
    stray = (place % TILE == REST) & (which < REST)
    weights[4] = window(which - REST * earlier + (block + TILE) * later, stray).astype(jnp.bfloat16)

    @pl.when(ends)
    def _():
        for i, (shift, which_core, center) in enumerate(((0, core, 1.0), (block * (earlier - later), 1 - core, 0.0))):
            base = TILE + TILE * which_core + shift
            spots = (
                (place + base - TILE, True), (place + base, place < REST), (which + base, stray),
                (place + DAY_HALF * (1 - which_core) + shift, True),
            )
            for n, (position, valid) in enumerate(spots):
                peak = jnp.where((position == day_of) & valid, center * (2.0 * DAY_HALF + 1.0), 0.0)
                weights[5 + 4 * i + n] = (window(position, valid) + peak).astype(jnp.bfloat16)

    def dot(which, columns, values):
        return jnp.dot(weights[which, :, 0:columns], values, preferred_element_type=jnp.float32)

    def strip(first, tail, j):
        if j < STEP - 1:
            return dot(first, TILE, tail[TILE * j : TILE * (j + 1), :])
        return dot(first + 1, PACKED, tail[...])

    def term(group, _):
        for j in range(STEP):
            lon = STEP * group + j
            total = dot(0, block, own[lon]) + dot(1, block, near[lon])
            terms[lon] = total + dot(2, TILE, heads[lon]) + strip(3, tails.at[group], j)
        return _

    def wrap_term(group):
        for j in range(STEP):
            lon = STEP * group + j
            total = dot(2, TILE, heads[lon]) + strip(3, tails.at[group], j)
            total += dot(5, TILE, wrap_heads[j]) + strip(6, wrap_tails, j) + dot(8, TILE, wrap_rests[j])
            total += dot(9, TILE, side_heads[j]) + strip(10, side_tails, j) + dot(12, TILE, side_rests[j])
            terms[lon] = total

    arrive(near_all)
    lax.fori_loop(0, 2, lambda i, c: term(1 + final * i, c), 0)
    arrive(far_head[1], far_tail[1])
    term(2, 0)
    total = opening(terms, 1)
    corner = final // 2 + 1
    for g in range(2, final):
        arrive(far_head[g], far_tail[g])
        term(g + 1, 0)
        if g - 1 < groups - LATE:
            total = results(terms, done, g - 1, 0, total)
        if g == corner:
            arrive(east_head, west_head, east_tail, west_tail)

            @pl.when(plane != 0)
            def _():
                arrive(near_west)
                term(0, 0)

            @pl.when(plane != PLANES - 1)
            def _():
                arrive(near_east)
                term(groups + 1, 0)

            @pl.when(ends)
            def _():
                arrive(*sides)
                wrap_term((groups + 1) * wrapped)

            results(terms, done, 0, 0, opening(terms, 0))

    def finish(*copies):
        for copy in copies:
            copy.wait_send()

    each_plane(east_pass, west_pass, finish)

    @pl.when(eastmost)
    def _():
        finish(*east_part, *east_wrap)

    @pl.when(plane != PLANES - 1)
    def _():
        finish(to_east, near_east)

    @pl.when(plane == 0)
    def _():
        finish(*west_part, *west_wrap)

    @pl.when(plane != 0)
    def _():
        finish(to_west, near_west)

    @pl.when(ends)
    def _():
        finish(*sides)

    for copy in (near_all, east_head, west_head, east_tail, west_tail):
        copy.wait_send()
    for copy in far_head + far_tail:
        copy.wait_send()


def solution(mesh):
    lons, days = mesh.shape["lon"], mesh.shape["day"]

    def local(field):
        rows, count, columns = field.shape
        groups = count // STEP
        wide = count + 2 * STEP
        slots = 16 + 2 * groups + RELAYS
        wrap_edges = [(STEP, TILE, columns), (PACKED, columns), (STEP, TILE, columns)]
        done, terms = pl.pallas_call(
            functools.partial(kernel, lons, days),
            out_shape=(
                pltpu.VMEM((count - LATE * STEP, rows, columns), jnp.float32),
                pltpu.VMEM((wide, rows, columns), jnp.float32),
            ),
            in_specs=[pl.BlockSpec(memory_space=pltpu.HBM)],
            out_specs=(pl.BlockSpec(memory_space=pltpu.VMEM), pl.BlockSpec(memory_space=pltpu.VMEM)),
            scratch_shapes=[
                pltpu.VMEM((wide, rows, columns), jnp.bfloat16),
                pltpu.VMEM((wide, rows, columns), jnp.bfloat16),
                pltpu.VMEM((wide, TILE, columns), jnp.bfloat16),
                pltpu.VMEM((groups + 2, PACKED, columns), jnp.bfloat16),
                pltpu.VMEM((groups, PACKED, columns), jnp.bfloat16),
                pltpu.VMEM((13, rows, PACKED), jnp.bfloat16),
                pltpu.VMEM((SHARE, TILE, columns), jnp.bfloat16),
                pltpu.SemaphoreType.REGULAR((5,)),
                pltpu.VMEM((STEP, TILE, columns), jnp.bfloat16),
                *[pltpu.VMEM(edge, jnp.bfloat16) for edge in 2 * wrap_edges],
                pltpu.SemaphoreType.DMA,
                pltpu.SemaphoreType.DMA((slots,)),
                pltpu.SemaphoreType.DMA((slots,)),
            ],
            compiler_params=pltpu.CompilerParams(
                collective_id=0, has_side_effects=True, vmem_limit_bytes=44 * 1024 * 1024
            ),
            name="anomaly",
        )(jnp.transpose(field, (1, 0, 2)))
        result = pl.pallas_call(
            finishing,
            out_shape=jax.ShapeDtypeStruct((count, rows, columns), jnp.float32),
            in_specs=[pl.BlockSpec(memory_space=pltpu.VMEM)] * 2,
            out_specs=pl.BlockSpec(memory_space=pl.ANY),
            scratch_shapes=[
                pltpu.VMEM((LATE * STEP, rows, columns), jnp.float32),
                pltpu.SemaphoreType.DMA((groups,)),
            ],
            compiler_params=pltpu.CompilerParams(vmem_limit_bytes=24 * 1024 * 1024),
            name="finishing",
        )(done, terms)
        return jnp.transpose(result, (1, 0, 2))

    return jax.shard_map(
        local, mesh=mesh, in_specs=(P("day", "lon", None),), out_specs=P("day", "lon", None), check_vma=False
    )
```

```python
import functools

import jax
import jax.numpy as jnp
from jax import lax
from jax.experimental import pallas as pl
from jax.experimental.pallas import tpu as pltpu
from jax.sharding import PartitionSpec as P

DAY_HALF = 15
LON_HALF = 10
PLANES = 8
TILE = 8
REST = DAY_HALF - TILE
STEP = LON_HALF
PACKED = (STEP - 1) * TILE
SCALE = 1.0 / ((2 * DAY_HALF + 1) * (2 * LON_HALF + 1))
RELAYS = 3
LATE = 3
SHARE = 3
KEPT = STEP - RELAYS * SHARE
MESH = pl.DeviceIdType.MESH


def product(weights, which, columns, values):
    return jnp.dot(weights[which, :, 0:columns], values, preferred_element_type=jnp.float32)


def strips(weights, first, tail, j):
    if j < STEP - 1:
        return product(weights, first, TILE, tail[TILE * j : TILE * (j + 1), :])
    return product(weights, first + 1, PACKED, tail[...])


def group_terms(group, weights, own, near, heads, tails, terms):
    block = own.shape[1]
    for j in range(STEP):
        lon = STEP * group + j
        total = product(weights, 0, block, own[lon]) + product(weights, 1, block, near[lon])
        terms[lon] = total + product(weights, 2, TILE, heads[lon]) + strips(weights, 3, tails.at[group], j)


def results(terms, target, group, first, total):
    def result(lon, total):
        total = total + terms[lon + 2 * STEP]
        target[lon - STEP * first] = total * SCALE
        return total - terms[lon]

    return lax.fori_loop(STEP * group, STEP * (group + 1), result, total)


def opening(terms, group):
    zero = jnp.zeros(terms.shape[1:], jnp.float32)
    return lax.fori_loop(STEP * group, STEP * (group + 2), lambda lon, total: total + terms[lon], zero)


def finishing(done, terms, heads, tails, weights, out, fresh, late, sems):
    early = done.shape[0] // STEP

    def put(source, group, first):
        return pltpu.make_async_copy(
            source.at[pl.ds(STEP * (group - first), STEP)], out.at[pl.ds(STEP * group, STEP)], sems.at[group]
        )

    copies = [put(done, group, 0) for group in range(early)]
    for copy in copies:
        copy.start()
    zero = jnp.zeros(terms.shape[1:], jnp.float32)
    total = lax.fori_loop(STEP * early, STEP * (early + 2), lambda lon, total: total + terms[lon], zero)
    for j in range(STEP):
        far = product(weights, 2, TILE, heads[j]) + strips(weights, 3, tails, j)
        fresh[j] = terms[STEP * (early + 2) + j] + far
    for group in range(early, early + LATE):

        def result(i, total):
            lon = STEP * group + i
            total = total + (fresh[i] if group == early else terms[lon + 2 * STEP])
            late[lon - STEP * early] = total * SCALE
            return total - (fresh[i] if group == early + 2 else terms[lon])

        total = lax.fori_loop(0, STEP, result, total)
        copies.append(put(late, group, early))
        copies[-1].start()
    for copy in copies:
        copy.wait()


def kernel(
    lons, days, field, done, terms, last_heads, last_tails, weights, own, near, heads, tails, packed, relayed, ready,
    apart, wrap_heads, wrap_tails, wrap_rests, side_heads, side_tails, side_rests, local_sem, send, recv,
):
    count = field.shape[0]
    columns = field.shape[2]
    groups = count // STEP
    here = lax.axis_index("lon")
    day = lax.axis_index("day")
    core = lax.rem(day, 2)
    turn = 2 * core - 1
    far_day = lax.rem(day + turn + days, days)
    near_day = lax.rem(day - turn + days, days)
    east = lax.rem(here + 1, lons)
    west = lax.rem(here + lons - 1, lons)
    plane = lax.rem(here, PLANES)

    barrier = pltpu.get_barrier_semaphore()

    def level(offset):
        return lax.rem(here + offset + lons, lons)

    def greet(*partners):
        for partner in partners:
            pl.semaphore_signal(barrier, inc=1, device_id=partner, device_id_type=MESH)

    reach = range(1, RELAYS + 1)
    eastmost = plane == PLANES - 1

    def at(spot):
        return functools.partial(pl.when, plane == spot)

    greet((here, far_day), (here, near_day))
    pl.when(plane != PLANES - 1)(functools.partial(greet, (east, day)))
    at(0)()(
        functools.partial(
            greet, (west, day), (west, far_day), *[(level(k), day) for k in reach[1:]], *[(level(-k - 1), day) for k in reach]
        )
    )
    for k in reach[1:]:
        at(PLANES - 1 - k)()(functools.partial(greet, (level(k), day)))
    load = pltpu.make_async_copy(field, own.at[pl.ds(STEP, count)], local_sem)
    load.start()
    waits = {0: 2, 1: 3, PLANES - 1: 4 + RELAYS}
    for spot in range(PLANES):
        at(spot)()(functools.partial(pl.semaphore_wait, barrier, waits.get(spot, 4)))

    def tell(slot, *partners):
        for partner in partners:
            pl.semaphore_signal(ready.at[slot], inc=1, device_id=partner, device_id_type=MESH)

    pl.when(plane != 0)(functools.partial(tell, 0, (west, day)))

    @pl.when(eastmost)
    def _():
        tell(1, (east, day))
        tell(2, (east, far_day))
        tell(3, *[(level(-k), day) for k in reach[1:]])

    for k in reach:
        at(PLANES - 1 - k)()(functools.partial(tell, 4, (level(k + 1), day)))
        at(k)()(functools.partial(tell, 5, (level(-k), day)))

    def remote(source, target, slot, device, sent=None):
        return pltpu.make_async_remote_copy(
            src_ref=source, dst_ref=target, send_sem=send.at[slot if sent is None else sent], recv_sem=recv.at[slot],
            device_id=device, device_id_type=MESH,
        )

    def start(*copies):
        for copy in copies:
            copy.start()

    def arrive(*copies):
        for copy in copies:
            copy.wait_recv()

    def span(group):
        return pl.ds(STEP * group, STEP)

    head_rows = pl.ds(pl.multiple_of(TILE * core, TILE), TILE)
    final = groups - 1

    to_east = remote(field.at[span(final)], own.at[span(0)], 0, (east, day))
    to_west = remote(field.at[span(0)], own.at[span(groups + 1)], 1, (west, day))
    near_all = remote(field, near.at[pl.ds(STEP, count)], 2, (here, near_day))
    near_west = remote(own.at[span(0)], near.at[span(0)], 3, (here, near_day))
    near_east = remote(own.at[span(groups + 1)], near.at[span(groups + 1)], 4, (here, near_day))
    east_head_direct = remote(field.at[span(final), head_rows], heads.at[span(0)], 5, (east, far_day))
    west_head_direct = remote(field.at[span(0), head_rows], heads.at[span(groups + 1)], 6, (west, far_day))
    east_tail_direct = remote(packed.at[final], tails.at[0], 7, (east, far_day))
    west_tail_direct = remote(packed.at[0], tails.at[groups + 1], 8, (west, far_day))
    east_head = remote(heads.at[span(groups)], heads.at[span(0)], 5, (east, day))
    west_head = remote(heads.at[span(1)], heads.at[span(groups + 1)], 6, (west, day))
    east_tail = remote(tails.at[groups], tails.at[0], 7, (east, day))
    west_tail = remote(tails.at[1], tails.at[groups + 1], 8, (west, day))
    spot = 9 + 2 * groups
    cut = [pl.ds(KEPT + SHARE * (k - 1), SHARE) for k in reach]
    kept = pl.ds(0, KEPT)

    turned = spot + RELAYS + 1
    east_part = [remote(apart.at[kept], wrap_rests.at[kept], turned, (east, day))]
    east_part += [remote(apart.at[cut[k - 1]], relayed, spot, (level(k + 1), day), spot + k) for k in reach]
    west_part = [remote(apart.at[kept], wrap_rests.at[kept], turned, (west, day))]
    west_part += [remote(apart.at[cut[k - 1]], relayed, spot, (level(-k - 1), day), spot + k) for k in reach]
    east_pass = [remote(relayed, wrap_rests.at[cut[k - 1]], turned, (level(-k), day), spot) for k in reach]
    west_pass = [remote(relayed, wrap_rests.at[cut[k - 1]], turned, (level(k), day), spot) for k in reach]
    wrap_rest = remote(apart, wrap_rests, turned, (east, day))
    east_wrap = (
        remote(heads.at[span(groups)], wrap_heads, turned + 1, (east, far_day)),
        remote(tails.at[groups], wrap_tails, turned + 2, (east, far_day)),
    )
    west_wrap = (
        remote(heads.at[span(1)], wrap_heads, turned + 1, (west, far_day)),
        remote(tails.at[1], wrap_tails, turned + 2, (west, far_day)),
    )
    sides = tuple(
        remote(source, target, turned + 3 + i, (here, near_day))
        for i, (source, target) in enumerate(((wrap_heads, side_heads), (wrap_tails, side_tails), (wrap_rests, side_rests)))
    )

    def each_plane(eastward, westward, act):
        for k in reach:
            pl.when(plane == k)(functools.partial(act, eastward[k - 1]))
            pl.when(plane == PLANES - 1 - k)(functools.partial(act, westward[k - 1]))

    far_head = [
        remote(
            field.at[span(g), head_rows], last_heads if g == final - 1 else heads.at[span(g + 1)], 9 + g, (here, far_day)
        )
        for g in range(groups)
    ]
    far_tail = [
        remote(packed.at[g], last_tails if g == final - 1 else tails.at[g + 1], 9 + groups + g, (here, far_day))
        for g in range(groups)
    ]

    start(far_head[0], far_head[final])

    @pl.when(eastmost)
    def _():
        start(east_head_direct)

    @pl.when(plane != 0)
    def _():
        start(to_west)

    start(near_all)
    load.wait()

    def rest(lon):
        rows = pl.ds(pl.multiple_of(TILE + TILE * core, TILE), REST)
        return own[lon, rows, :].astype(jnp.float32)

    def pack(group, _):
        base = STEP * (group + 1)
        spare = rest(base + STEP - 1)
        for j in range(STEP - 1):
            extra = spare[j % REST : j % REST + 1]
            tile = jnp.concatenate([rest(base + j), extra], axis=0)
            packed[group, TILE * j : TILE * (j + 1), :] = tile.astype(jnp.bfloat16)
        return _

    lax.fori_loop(0, groups, pack, 0)

    ends = (plane == 0) | eastmost
    wrapped = plane // (PLANES - 1)

    @pl.when(ends)
    def _():
        def part(j, _):
            lon = STEP + STEP * final * wrapped + j
            low = own[lon, 0:TILE, :].astype(jnp.float32)
            high = own[lon, TILE:, :].astype(jnp.float32)
            apart[j] = jnp.where(core == 0, high[REST:], low).astype(jnp.bfloat16)
            return _

        lax.fori_loop(0, STEP, part, 0)

    start(far_tail[0], far_tail[final])

    @pl.when(eastmost)
    def _():
        start(east_part[0], east_tail_direct)

    for g in range(1, final):
        start(far_head[g], far_tail[g])

    @pl.when(plane != PLANES - 1)
    def _():
        pl.semaphore_wait(ready.at[0], 1)
        start(to_east)

    @pl.when(plane == 0)
    def _():
        pl.semaphore_wait(ready.at[1], 1)
        pl.semaphore_wait(ready.at[5], RELAYS)
        tell(6, (west, day))
        pl.semaphore_wait(ready.at[2], 1)
        pl.semaphore_wait(ready.at[4], RELAYS)
        start(*west_part, west_head_direct, west_tail_direct)

    @pl.when(eastmost)
    def _():
        pl.semaphore_wait(ready.at[6], 1)
        start(*east_part[1:])

    for k in reach[1:]:
        at(PLANES - 1 - k)()(functools.partial(pl.semaphore_wait, ready.at[3], 1))

    def forward(copy):
        arrive(east_part[1])
        start(copy)

    each_plane(east_pass, west_pass, forward)

    @pl.when(plane != 0)
    def _():
        arrive(to_east)
        start(near_west)

    @pl.when(plane != PLANES - 1)
    def _():
        arrive(to_west)
        start(near_east)

    arrive(far_head[0], far_head[final], far_tail[0], far_tail[final])

    @pl.when(plane != PLANES - 1)
    def _():
        start(east_head, east_tail)

    @pl.when(plane != 0)
    def _():
        start(west_head, west_tail)

    @pl.when(eastmost)
    def _():
        start(*east_wrap)

    @pl.when(plane == 0)
    def _():
        start(*west_wrap)

    @pl.when(ends)
    def _():
        arrive(wrap_rest, *east_wrap)
        start(*sides)

    day_of = lax.broadcasted_iota(jnp.int32, weights.shape[1:], 0)
    place = lax.broadcasted_iota(jnp.int32, weights.shape[1:], 1)

    def window(position, valid=True):
        inside = (jnp.abs(position - day_of) <= DAY_HALF) & valid
        return jnp.where(inside, -1.0, 0.0)

    block = own.shape[1]
    earlier, later = 1 - core, core
    weights[0] = (window(place) + jnp.where(place == day_of, 2.0 * DAY_HALF + 1.0, 0.0)).astype(jnp.bfloat16)
    weights[1] = window(place + block * (earlier - later)).astype(jnp.bfloat16)
    weights[2] = window(place - DAY_HALF * earlier + block * later).astype(jnp.bfloat16)
    weights[3] = window(place - REST * earlier + (block + TILE) * later, place < REST).astype(jnp.bfloat16)
    which = place // TILE
    stray = (place % TILE == REST) & (which < REST)
    weights[4] = window(which - REST * earlier + (block + TILE) * later, stray).astype(jnp.bfloat16)

    @pl.when(ends)
    def _():
        for i, (shift, which_core, center) in enumerate(((0, core, 1.0), (block * (earlier - later), 1 - core, 0.0))):
            base = TILE + TILE * which_core + shift
            spots = (
                (place + base - TILE, True), (place + base, place < REST), (which + base, stray),
                (place + DAY_HALF * (1 - which_core) + shift, True),
            )
            for n, (position, valid) in enumerate(spots):
                peak = jnp.where((position == day_of) & valid, center * (2.0 * DAY_HALF + 1.0), 0.0)
                weights[5 + 4 * i + n] = (window(position, valid) + peak).astype(jnp.bfloat16)

    dot, strip = functools.partial(product, weights), functools.partial(strips, weights)

    def term(group, _):
        group_terms(group, weights, own, near, heads, tails, terms)
        return _

    def wrap_term(group):
        for j in range(STEP):
            lon = STEP * group + j
            total = dot(2, TILE, heads[lon]) + strip(3, tails.at[group], j)
            total += dot(5, TILE, wrap_heads[j]) + strip(6, wrap_tails, j) + dot(8, TILE, wrap_rests[j])
            total += dot(9, TILE, side_heads[j]) + strip(10, side_tails, j) + dot(12, TILE, side_rests[j])
            terms[lon] = total

    arrive(near_all)
    lax.fori_loop(0, 2, lambda i, c: term(1 + final * i, c), 0)
    arrive(far_head[1], far_tail[1])
    term(2, 0)
    total = opening(terms, 1)
    corner = final // 2 + 1
    for g in range(2, final):
        if g < final - 1:
            arrive(far_head[g], far_tail[g])
            term(g + 1, 0)
        else:
            for lon in range(STEP * (g + 1), STEP * (g + 2)):
                terms[lon] = dot(0, block, own[lon]) + dot(1, block, near[lon])
            arrive(far_head[g], far_tail[g])
        if g - 1 < groups - LATE:
            total = results(terms, done, g - 1, 0, total)
        if g == corner:
            arrive(east_head, west_head, east_tail, west_tail)

            @pl.when(plane != 0)
            def _():
                arrive(near_west)
                term(0, 0)

            @pl.when(plane != PLANES - 1)
            def _():
                arrive(near_east)
                term(groups + 1, 0)

            @pl.when(ends)
            def _():
                arrive(*sides)
                wrap_term((groups + 1) * wrapped)

            results(terms, done, 0, 0, opening(terms, 0))

    def finish(*copies):
        for copy in copies:
            copy.wait_send()

    each_plane(east_pass, west_pass, finish)

    @pl.when(eastmost)
    def _():
        finish(*east_part, *east_wrap)

    @pl.when(plane != PLANES - 1)
    def _():
        finish(to_east, near_east)

    @pl.when(plane == 0)
    def _():
        finish(*west_part, *west_wrap)

    @pl.when(plane != 0)
    def _():
        finish(to_west, near_west)

    @pl.when(ends)
    def _():
        finish(*sides)

    for copy in (near_all, east_head, west_head, east_tail, west_tail):
        copy.wait_send()
    for copy in far_head + far_tail:
        copy.wait_send()


def solution(mesh):
    lons, days = mesh.shape["lon"], mesh.shape["day"]

    def local(field):
        rows, count, columns = field.shape
        groups = count // STEP
        wide = count + 2 * STEP
        slots = 16 + 2 * groups + RELAYS
        wrap_edges = [(STEP, TILE, columns), (PACKED, columns), (STEP, TILE, columns)]
        vmem = pl.BlockSpec(memory_space=pltpu.VMEM)
        gathered = pl.pallas_call(
            functools.partial(kernel, lons, days),
            out_shape=(
                pltpu.VMEM((count - LATE * STEP, rows, columns), jnp.float32),
                pltpu.VMEM((wide, rows, columns), jnp.float32),
                pltpu.VMEM((STEP, TILE, columns), jnp.bfloat16),
                pltpu.VMEM((PACKED, columns), jnp.bfloat16),
                pltpu.VMEM((13, rows, PACKED), jnp.bfloat16),
            ),
            in_specs=[pl.BlockSpec(memory_space=pltpu.HBM)],
            out_specs=(vmem,) * 5,
            scratch_shapes=[
                pltpu.VMEM((wide, rows, columns), jnp.bfloat16),
                pltpu.VMEM((wide, rows, columns), jnp.bfloat16),
                pltpu.VMEM((wide, TILE, columns), jnp.bfloat16),
                pltpu.VMEM((groups + 2, PACKED, columns), jnp.bfloat16),
                pltpu.VMEM((groups, PACKED, columns), jnp.bfloat16),
                pltpu.VMEM((SHARE, TILE, columns), jnp.bfloat16),
                pltpu.SemaphoreType.REGULAR((7,)),
                pltpu.VMEM((STEP, TILE, columns), jnp.bfloat16),
                *[pltpu.VMEM(edge, jnp.bfloat16) for edge in 2 * wrap_edges],
                pltpu.SemaphoreType.DMA,
                pltpu.SemaphoreType.DMA((slots,)),
                pltpu.SemaphoreType.DMA((slots,)),
            ],
            compiler_params=pltpu.CompilerParams(
                collective_id=0, has_side_effects=True, vmem_limit_bytes=40 * 1024 * 1024
            ),
            name="anomaly",
        )(jnp.transpose(field, (1, 0, 2)))
        result = pl.pallas_call(
            finishing,
            out_shape=jax.ShapeDtypeStruct((count, rows, columns), jnp.float32),
            in_specs=[vmem] * 5,
            out_specs=pl.BlockSpec(memory_space=pl.ANY),
            scratch_shapes=[
                pltpu.VMEM((STEP, rows, columns), jnp.float32),
                pltpu.VMEM((LATE * STEP, rows, columns), jnp.float32),
                pltpu.SemaphoreType.DMA((groups,)),
            ],
            compiler_params=pltpu.CompilerParams(vmem_limit_bytes=16 * 1024 * 1024),
            name="finishing",
        )(*gathered)
        return jnp.transpose(result, (1, 0, 2))

    return jax.shard_map(
        local, mesh=mesh, in_specs=(P("day", "lon", None),), out_specs=P("day", "lon", None), check_vma=False
    )
```

```python
import functools

import jax
import jax.numpy as jnp
from jax import lax
from jax.experimental import pallas as pl
from jax.experimental.pallas import tpu as pltpu
from jax.sharding import PartitionSpec as P

DAY_HALF = 15
LON_HALF = 10
PLANES = 8
TILE = 8
REST = DAY_HALF - TILE
STEP = LON_HALF
PACKED = (STEP - 1) * TILE
DENSE = REST * TILE
SCALE = 1.0 / ((2 * DAY_HALF + 1) * (2 * LON_HALF + 1))
RELAYS = 3
LATE = 3
SHARE = 3
KEPT = STEP - RELAYS * SHARE
MESH = pl.DeviceIdType.MESH


def product(weights, which, columns, values):
    return jnp.dot(weights[which, :, 0:columns], values, preferred_element_type=jnp.float32)


def strips(weights, first, tail, j):
    if j < STEP - 1:
        return product(weights, first, TILE, tail[TILE * j : TILE * (j + 1), :])
    return product(weights, first + 1, PACKED, tail[...])


def group_terms(group, weights, own, near, heads, tails, terms, moved=None):
    block = own.shape[1]
    for j in range(STEP):
        lon = STEP * group + j
        total = product(weights, 0, block, own[lon]) + product(weights, 1, block, near[lon])
        total += product(weights, 2, TILE, heads[lon])
        if moved is None or j < REST:
            total += strips(weights, 3, tails.at[group], j)
        else:
            rows = tails[group, 0:DENSE, :] if j == STEP - 1 else moved[j - REST]
            total += product(weights, 4, DENSE, rows)
        terms[lon] = total


def results(terms, target, group, first, total):
    def result(lon, total):
        total = total + terms[lon + 2 * STEP]
        target[lon - STEP * first] = total * SCALE
        return total - terms[lon]

    return lax.fori_loop(STEP * group, STEP * (group + 1), result, total)


def opening(terms, group):
    zero = jnp.zeros(terms.shape[1:], jnp.float32)
    return lax.fori_loop(STEP * group, STEP * (group + 2), lambda lon, total: total + terms[lon], zero)


def finishing(done, terms, heads, tails, weights, out, fresh, late, sems):
    early = done.shape[0] // STEP

    def put(source, group, first):
        return pltpu.make_async_copy(
            source.at[pl.ds(STEP * (group - first), STEP)], out.at[pl.ds(STEP * group, STEP)], sems.at[group]
        )

    copies = [put(done, group, 0) for group in range(early)]
    for copy in copies:
        copy.start()
    zero = jnp.zeros(terms.shape[1:], jnp.float32)
    total = lax.fori_loop(STEP * early, STEP * (early + 2), lambda lon, total: total + terms[lon], zero)
    for j in range(STEP):
        far = product(weights, 2, TILE, heads[j]) + strips(weights, 3, tails, j)
        fresh[j] = terms[STEP * (early + 2) + j] + far
    for group in range(early, early + LATE):

        def result(i, total):
            lon = STEP * group + i
            total = total + (fresh[i] if group == early else terms[lon + 2 * STEP])
            late[lon - STEP * early] = total * SCALE
            return total - (fresh[i] if group == early + 2 else terms[lon])

        total = lax.fori_loop(0, STEP, result, total)
        copies.append(put(late, group, early))
        copies[-1].start()
    for copy in copies:
        copy.wait()


def kernel(
    lons, days, field, done, terms, last_heads, last_tails, weights, own, near, heads, tails, packed, strayed, moved, relayed, ready,
    apart, wrap_heads, wrap_tails, wrap_rests, side_heads, side_tails, side_rests, local_sem, send, recv,
):
    count = field.shape[0]
    columns = field.shape[2]
    groups = count // STEP
    here = lax.axis_index("lon")
    day = lax.axis_index("day")
    core = lax.rem(day, 2)
    turn = 2 * core - 1
    far_day = lax.rem(day + turn + days, days)
    near_day = lax.rem(day - turn + days, days)
    east = lax.rem(here + 1, lons)
    west = lax.rem(here + lons - 1, lons)
    plane = lax.rem(here, PLANES)

    barrier = pltpu.get_barrier_semaphore()

    def level(offset):
        return lax.rem(here + offset + lons, lons)

    def greet(*partners):
        for partner in partners:
            pl.semaphore_signal(barrier, inc=1, device_id=partner, device_id_type=MESH)

    reach = range(1, RELAYS + 1)
    eastmost = plane == PLANES - 1

    def at(spot):
        return functools.partial(pl.when, plane == spot)

    greet((here, far_day), (here, near_day))
    pl.when(plane != PLANES - 1)(functools.partial(greet, (east, day)))
    at(0)()(
        functools.partial(
            greet, (west, day), (west, far_day), *[(level(k), day) for k in reach[1:]], *[(level(-k - 1), day) for k in reach]
        )
    )
    for k in reach[1:]:
        at(PLANES - 1 - k)()(functools.partial(greet, (level(k), day)))
    load = pltpu.make_async_copy(field, own.at[pl.ds(STEP, count)], local_sem)
    load.start()
    waits = {0: 2, 1: 3, PLANES - 1: 4 + RELAYS}
    for spot in range(PLANES):
        at(spot)()(functools.partial(pl.semaphore_wait, barrier, waits.get(spot, 4)))

    def tell(slot, *partners):
        for partner in partners:
            pl.semaphore_signal(ready.at[slot], inc=1, device_id=partner, device_id_type=MESH)

    pl.when(plane != 0)(functools.partial(tell, 0, (west, day)))

    @pl.when(eastmost)
    def _():
        tell(1, (east, day))
        tell(2, (east, far_day))
        tell(3, *[(level(-k), day) for k in reach[1:]])

    for k in reach:
        at(PLANES - 1 - k)()(functools.partial(tell, 4, (level(k + 1), day)))
        at(k)()(functools.partial(tell, 5, (level(-k), day)))

    def remote(source, target, slot, device, sent=None):
        return pltpu.make_async_remote_copy(
            src_ref=source, dst_ref=target, send_sem=send.at[slot if sent is None else sent], recv_sem=recv.at[slot],
            device_id=device, device_id_type=MESH,
        )

    def start(*copies):
        for copy in copies:
            copy.start()

    def arrive(*copies):
        for copy in copies:
            copy.wait_recv()

    def span(group):
        return pl.ds(STEP * group, STEP)

    head_rows = pl.ds(pl.multiple_of(TILE * core, TILE), TILE)
    final = groups - 1
    thin = final - 2
    holders = (0, final, *range(1, REST - 1))

    to_east = remote(field.at[span(final)], own.at[span(0)], 0, (east, day))
    to_west = remote(field.at[span(0)], own.at[span(groups + 1)], 1, (west, day))
    near_all = remote(field, near.at[pl.ds(STEP, count)], 2, (here, near_day))
    near_west = remote(own.at[span(0)], near.at[span(0)], 3, (here, near_day))
    near_east = remote(own.at[span(groups + 1)], near.at[span(groups + 1)], 4, (here, near_day))
    east_head_direct = remote(field.at[span(final), head_rows], heads.at[span(0)], 5, (east, far_day))
    west_head_direct = remote(field.at[span(0), head_rows], heads.at[span(groups + 1)], 6, (west, far_day))
    east_tail_direct = remote(packed.at[final], tails.at[0], 7, (east, far_day))
    west_tail_direct = remote(packed.at[0], tails.at[groups + 1], 8, (west, far_day))
    east_head = remote(heads.at[span(groups)], heads.at[span(0)], 5, (east, day))
    west_head = remote(heads.at[span(1)], heads.at[span(groups + 1)], 6, (west, day))
    east_tail = remote(tails.at[groups], tails.at[0], 7, (east, day))
    west_tail = remote(tails.at[1], tails.at[groups + 1], 8, (west, day))
    spot = 9 + 2 * groups
    cut = [pl.ds(KEPT + SHARE * (k - 1), SHARE) for k in reach]
    kept = pl.ds(0, KEPT)

    turned = spot + RELAYS + 1
    east_part = [remote(apart.at[kept], wrap_rests.at[kept], turned, (east, day))]
    east_part += [remote(apart.at[cut[k - 1]], relayed, spot, (level(k + 1), day), spot + k) for k in reach]
    west_part = [remote(apart.at[kept], wrap_rests.at[kept], turned, (west, day))]
    west_part += [remote(apart.at[cut[k - 1]], relayed, spot, (level(-k - 1), day), spot + k) for k in reach]
    east_pass = [remote(relayed, wrap_rests.at[cut[k - 1]], turned, (level(-k), day), spot) for k in reach]
    west_pass = [remote(relayed, wrap_rests.at[cut[k - 1]], turned, (level(k), day), spot) for k in reach]
    wrap_rest = remote(apart, wrap_rests, turned, (east, day))
    east_wrap = (
        remote(heads.at[span(groups)], wrap_heads, turned + 1, (east, far_day)),
        remote(tails.at[groups], wrap_tails, turned + 2, (east, far_day)),
    )
    west_wrap = (
        remote(heads.at[span(1)], wrap_heads, turned + 1, (west, far_day)),
        remote(tails.at[1], wrap_tails, turned + 2, (west, far_day)),
    )
    sides = tuple(
        remote(source, target, turned + 3 + i, (here, near_day))
        for i, (source, target) in enumerate(((wrap_heads, side_heads), (wrap_tails, side_tails), (wrap_rests, side_rests)))
    )

    def each_plane(eastward, westward, act):
        for k in reach:
            pl.when(plane == k)(functools.partial(act, eastward[k - 1]))
            pl.when(plane == PLANES - 1 - k)(functools.partial(act, westward[k - 1]))

    far_head = [
        remote(
            field.at[span(g), head_rows], last_heads if g == final - 1 else heads.at[span(g + 1)], 9 + g, (here, far_day)
        )
        for g in range(groups)
    ]
    far_tail = [
        remote(
            packed.at[g, pl.ds(0, DENSE)] if g == thin else packed.at[g],
            last_tails if g == final - 1 else tails.at[g + 1, pl.ds(0, DENSE)] if g == thin else tails.at[g + 1],
            9 + groups + g, (here, far_day),
        )
        for g in range(groups)
    ]

    start(far_head[0], far_head[final])

    @pl.when(eastmost)
    def _():
        start(east_head_direct)

    @pl.when(plane != 0)
    def _():
        start(to_west)

    start(near_all)
    load.wait()

    def rest(lon):
        rows = pl.ds(pl.multiple_of(TILE + TILE * core, TILE), REST)
        return own[lon, rows, :].astype(jnp.float32)

    for i in range(STEP - 1 - REST):
        strayed[i, 0:REST, :] = rest(STEP * (thin + 1) + REST + i)

    def pack(group, _):
        base = STEP * (group + 1)
        spare = rest(base + STEP - 1)
        row = jnp.where(group == 0, 0, jnp.where(group == final, 1, jnp.minimum(group + 1, REST - 1)))
        for j in range(STEP - 1):
            extra = spare[j : j + 1] if j < REST else strayed[j - REST, pl.ds(row, 1), :]
            tile = jnp.concatenate([rest(base + j), extra], axis=0)
            packed[group, TILE * j : TILE * (j + 1), :] = tile.astype(jnp.bfloat16)
        return _

    lax.fori_loop(0, groups, pack, 0)

    ends = (plane == 0) | eastmost
    wrapped = plane // (PLANES - 1)

    @pl.when(ends)
    def _():
        def part(j, _):
            lon = STEP + STEP * final * wrapped + j
            low = own[lon, 0:TILE, :].astype(jnp.float32)
            high = own[lon, TILE:, :].astype(jnp.float32)
            apart[j] = jnp.where(core == 0, high[REST:], low).astype(jnp.bfloat16)
            return _

        lax.fori_loop(0, STEP, part, 0)

    start(far_tail[0], far_tail[final])

    @pl.when(eastmost)
    def _():
        start(east_part[0], east_tail_direct)

    for g in range(1, final):
        start(far_head[g], far_tail[g])

    @pl.when(plane != PLANES - 1)
    def _():
        pl.semaphore_wait(ready.at[0], 1)
        start(to_east)

    @pl.when(plane == 0)
    def _():
        pl.semaphore_wait(ready.at[1], 1)
        pl.semaphore_wait(ready.at[5], RELAYS)
        tell(6, (west, day))
        pl.semaphore_wait(ready.at[2], 1)
        pl.semaphore_wait(ready.at[4], RELAYS)
        start(*west_part, west_head_direct, west_tail_direct)

    @pl.when(eastmost)
    def _():
        pl.semaphore_wait(ready.at[6], 1)
        start(*east_part[1:])

    for k in reach[1:]:
        at(PLANES - 1 - k)()(functools.partial(pl.semaphore_wait, ready.at[3], 1))

    def forward(copy):
        arrive(east_part[1])
        start(copy)

    each_plane(east_pass, west_pass, forward)

    @pl.when(plane != 0)
    def _():
        arrive(to_east)
        start(near_west)

    @pl.when(plane != PLANES - 1)
    def _():
        arrive(to_west)
        start(near_east)

    arrive(far_head[0], far_head[final], far_tail[0], far_tail[final])

    @pl.when(plane != PLANES - 1)
    def _():
        start(east_head, east_tail)

    @pl.when(plane != 0)
    def _():
        start(west_head, west_tail)

    @pl.when(eastmost)
    def _():
        start(*east_wrap)

    @pl.when(plane == 0)
    def _():
        start(*west_wrap)

    @pl.when(ends)
    def _():
        arrive(wrap_rest, *east_wrap)
        start(*sides)

    day_of = lax.broadcasted_iota(jnp.int32, weights.shape[1:], 0)
    place = lax.broadcasted_iota(jnp.int32, weights.shape[1:], 1)

    def window(position, valid=True):
        inside = (jnp.abs(position - day_of) <= DAY_HALF) & valid
        return jnp.where(inside, -1.0, 0.0)

    block = own.shape[1]
    earlier, later = 1 - core, core
    weights[0] = (window(place) + jnp.where(place == day_of, 2.0 * DAY_HALF + 1.0, 0.0)).astype(jnp.bfloat16)
    weights[1] = window(place + block * (earlier - later)).astype(jnp.bfloat16)
    weights[2] = window(place - DAY_HALF * earlier + block * later).astype(jnp.bfloat16)
    weights[3] = window(place - REST * earlier + (block + TILE) * later, place < REST).astype(jnp.bfloat16)
    which = place // TILE
    stray = (place % TILE == REST) & (which < REST)
    weights[4] = window(which - REST * earlier + (block + TILE) * later, stray).astype(jnp.bfloat16)

    @pl.when(ends)
    def _():
        for i, (shift, which_core, center) in enumerate(((0, core, 1.0), (block * (earlier - later), 1 - core, 0.0))):
            base = TILE + TILE * which_core + shift
            spots = (
                (place + base - TILE, True), (place + base, place < REST), (which + base, stray),
                (place + DAY_HALF * (1 - which_core) + shift, True),
            )
            for n, (position, valid) in enumerate(spots):
                peak = jnp.where((position == day_of) & valid, center * (2.0 * DAY_HALF + 1.0), 0.0)
                weights[5 + 4 * i + n] = (window(position, valid) + peak).astype(jnp.bfloat16)

    dot, strip = functools.partial(product, weights), functools.partial(strips, weights)

    def term(group, _):
        group_terms(group, weights, own, near, heads, tails, terms)
        return _

    def wrap_term(group):
        for j in range(STEP):
            lon = STEP * group + j
            total = dot(2, TILE, heads[lon]) + strip(3, tails.at[group], j)
            total += dot(5, TILE, wrap_heads[j]) + strip(6, wrap_tails, j) + dot(8, TILE, wrap_rests[j])
            total += dot(9, TILE, side_heads[j]) + strip(10, side_tails, j) + dot(12, TILE, side_rests[j])
            terms[lon] = total

    arrive(near_all)
    lax.fori_loop(0, 2, lambda i, c: term(1 + final * i, c), 0)
    arrive(far_head[1], far_tail[1])
    term(2, 0)
    total = opening(terms, 1)
    corner = final // 2 + 1
    for g in range(2, final):
        if g < final - 1:
            arrive(far_head[g], far_tail[g])
            if g == thin:
                for i in range(STEP - 1 - REST):
                    place_in = pl.ds(TILE * (REST + i), TILE)
                    for n, holder in enumerate(holders):
                        moved[i, TILE * n : TILE * (n + 1), :] = tails[holder + 1, place_in, :]
                group_terms(g + 1, weights, own, near, heads, tails, terms, moved)
            else:
                term(g + 1, 0)
        else:
            for lon in range(STEP * (g + 1), STEP * (g + 2)):
                terms[lon] = dot(0, block, own[lon]) + dot(1, block, near[lon])
            arrive(far_head[g], far_tail[g])
        if g - 1 < groups - LATE:
            total = results(terms, done, g - 1, 0, total)
        if g == corner:
            arrive(east_head, west_head, east_tail, west_tail)

            @pl.when(plane != 0)
            def _():
                arrive(near_west)
                term(0, 0)

            @pl.when(plane != PLANES - 1)
            def _():
                arrive(near_east)
                term(groups + 1, 0)

            @pl.when(ends)
            def _():
                arrive(*sides)
                wrap_term((groups + 1) * wrapped)

            results(terms, done, 0, 0, opening(terms, 0))

    def finish(*copies):
        for copy in copies:
            copy.wait_send()

    each_plane(east_pass, west_pass, finish)

    @pl.when(eastmost)
    def _():
        finish(*east_part, *east_wrap)

    @pl.when(plane != PLANES - 1)
    def _():
        finish(to_east, near_east)

    @pl.when(plane == 0)
    def _():
        finish(*west_part, *west_wrap)

    @pl.when(plane != 0)
    def _():
        finish(to_west, near_west)

    @pl.when(ends)
    def _():
        finish(*sides)

    for copy in (near_all, east_head, west_head, east_tail, west_tail):
        copy.wait_send()
    for copy in far_head + far_tail:
        copy.wait_send()


def solution(mesh):
    lons, days = mesh.shape["lon"], mesh.shape["day"]

    def local(field):
        rows, count, columns = field.shape
        groups = count // STEP
        wide = count + 2 * STEP
        slots = 16 + 2 * groups + RELAYS
        wrap_edges = [(STEP, TILE, columns), (PACKED, columns), (STEP, TILE, columns)]
        vmem = pl.BlockSpec(memory_space=pltpu.VMEM)
        gathered = pl.pallas_call(
            functools.partial(kernel, lons, days),
            out_shape=(
                pltpu.VMEM((count - LATE * STEP, rows, columns), jnp.float32),
                pltpu.VMEM((wide, rows, columns), jnp.float32),
                pltpu.VMEM((STEP, TILE, columns), jnp.bfloat16),
                pltpu.VMEM((PACKED, columns), jnp.bfloat16),
                pltpu.VMEM((13, rows, PACKED), jnp.bfloat16),
            ),
            in_specs=[pl.BlockSpec(memory_space=pltpu.HBM)],
            out_specs=(vmem,) * 5,
            scratch_shapes=[
                pltpu.VMEM((wide, rows, columns), jnp.bfloat16),
                pltpu.VMEM((wide, rows, columns), jnp.bfloat16),
                pltpu.VMEM((wide, TILE, columns), jnp.bfloat16),
                pltpu.VMEM((groups + 2, PACKED, columns), jnp.bfloat16),
                pltpu.VMEM((groups, PACKED, columns), jnp.bfloat16),
                pltpu.VMEM((STEP - 1 - REST, TILE, columns), jnp.float32),
                pltpu.VMEM((STEP - 1 - REST, DENSE, columns), jnp.bfloat16),
                pltpu.VMEM((SHARE, TILE, columns), jnp.bfloat16),
                pltpu.SemaphoreType.REGULAR((7,)),
                pltpu.VMEM((STEP, TILE, columns), jnp.bfloat16),
                *[pltpu.VMEM(edge, jnp.bfloat16) for edge in 2 * wrap_edges],
                pltpu.SemaphoreType.DMA,
                pltpu.SemaphoreType.DMA((slots,)),
                pltpu.SemaphoreType.DMA((slots,)),
            ],
            compiler_params=pltpu.CompilerParams(
                collective_id=0, has_side_effects=True, vmem_limit_bytes=40 * 1024 * 1024
            ),
            name="anomaly",
        )(jnp.transpose(field, (1, 0, 2)))
        result = pl.pallas_call(
            finishing,
            out_shape=jax.ShapeDtypeStruct((count, rows, columns), jnp.float32),
            in_specs=[vmem] * 5,
            out_specs=pl.BlockSpec(memory_space=pl.ANY),
            scratch_shapes=[
                pltpu.VMEM((STEP, rows, columns), jnp.float32),
                pltpu.VMEM((LATE * STEP, rows, columns), jnp.float32),
                pltpu.SemaphoreType.DMA((groups,)),
            ],
            compiler_params=pltpu.CompilerParams(vmem_limit_bytes=16 * 1024 * 1024),
            name="finishing",
        )(*gathered)
        return jnp.transpose(result, (1, 0, 2))

    return jax.shard_map(
        local, mesh=mesh, in_specs=(P("day", "lon", None),), out_specs=P("day", "lon", None), check_vma=False
    )
```

```python
import functools

import jax
import jax.numpy as jnp
from jax import lax
from jax.experimental import pallas as pl
from jax.experimental.pallas import tpu as pltpu
from jax.sharding import PartitionSpec as P

DAY_HALF = 15
LON_HALF = 10
PLANES = 8
TILE = 8
REST = DAY_HALF - TILE
STEP = LON_HALF
PACKED = (STEP - 1) * TILE
DENSE = REST * TILE
SCALE = 1.0 / ((2 * DAY_HALF + 1) * (2 * LON_HALF + 1))
RELAYS = 3
LATE = 3
SHARE = 3
KEPT = STEP - RELAYS * SHARE
MESH = pl.DeviceIdType.MESH


def product(weights, which, columns, values):
    return jnp.dot(weights[which, :, 0:columns], values, preferred_element_type=jnp.float32)


def strips(weights, first, tail, j):
    if j < STEP - 1:
        return product(weights, first, TILE, tail[TILE * j : TILE * (j + 1), :])
    return product(weights, first + 1, PACKED, tail[...])


def group_terms(group, weights, own, near, heads, tails, terms, moved=None):
    block = own.shape[1]
    for j in range(STEP):
        lon = STEP * group + j
        total = product(weights, 0, block, own[lon]) + product(weights, 1, block, near[lon])
        total += product(weights, 2, TILE, heads[lon])
        if moved is None or j < REST:
            total += strips(weights, 3, tails.at[group], j)
        else:
            rows = tails[group, 0:DENSE, :] if j == STEP - 1 else moved[j - REST]
            total += product(weights, 4, DENSE, rows)
        terms[lon] = total


def results(terms, target, group, first, total):
    def result(lon, total):
        total = total + terms[lon + 2 * STEP]
        target[lon - STEP * first] = total * SCALE
        return total - terms[lon]

    return lax.fori_loop(STEP * group, STEP * (group + 1), result, total)


def opening(terms, group):
    zero = jnp.zeros(terms.shape[1:], jnp.float32)
    return lax.fori_loop(STEP * group, STEP * (group + 2), lambda lon, total: total + terms[lon], zero)


def finishing(done, terms, heads, tails, weights, out, fresh, late, sems):
    early = done.shape[0] // STEP

    def put(source, group, first):
        return pltpu.make_async_copy(
            source.at[pl.ds(STEP * (group - first), STEP)], out.at[pl.ds(STEP * group, STEP)], sems.at[group]
        )

    copies = [put(done, group, 0) for group in range(early)]
    for copy in copies:
        copy.start()
    zero = jnp.zeros(terms.shape[1:], jnp.float32)
    total = lax.fori_loop(STEP * early, STEP * (early + 2), lambda lon, total: total + terms[lon], zero)
    for j in range(STEP):
        far = product(weights, 2, TILE, heads[j]) + strips(weights, 3, tails, j)
        fresh[j] = terms[STEP * (early + 2) + j] + far
    for group in range(early, early + LATE):

        def result(i, total):
            lon = STEP * group + i
            total = total + (fresh[i] if group == early else terms[lon + 2 * STEP])
            late[lon - STEP * early] = total * SCALE
            return total - (fresh[i] if group == early + 2 else terms[lon])

        total = lax.fori_loop(0, STEP, result, total)
        copies.append(put(late, group, early))
        copies[-1].start()
    for copy in copies:
        copy.wait()


def kernel(
    lons, days, field, done, terms, last_heads, last_tails, weights, own, near, heads, tails, packed, strayed, moved, relayed, ready,
    apart, wrap_heads, wrap_tails, wrap_rests, side_heads, side_tails, side_rests, local_sem, send, recv,
):
    count = field.shape[0]
    columns = field.shape[2]
    groups = count // STEP
    here = lax.axis_index("lon")
    day = lax.axis_index("day")
    core = lax.rem(day, 2)
    turn = 2 * core - 1
    far_day = lax.rem(day + turn + days, days)
    near_day = lax.rem(day - turn + days, days)
    east = lax.rem(here + 1, lons)
    west = lax.rem(here + lons - 1, lons)
    plane = lax.rem(here, PLANES)

    barrier = pltpu.get_barrier_semaphore()

    def level(offset):
        return lax.rem(here + offset + lons, lons)

    def greet(*partners):
        for partner in partners:
            pl.semaphore_signal(barrier, inc=1, device_id=partner, device_id_type=MESH)

    reach = range(1, RELAYS + 1)
    eastmost = plane == PLANES - 1

    def at(spot):
        return functools.partial(pl.when, plane == spot)

    greet((here, far_day), (here, near_day))
    pl.when(plane != PLANES - 1)(functools.partial(greet, (east, day)))
    at(0)()(
        functools.partial(
            greet, (west, day), *[(level(k), day) for k in reach[1:]]
        )
    )
    for k in reach[1:]:
        at(PLANES - 1 - k)()(functools.partial(greet, (level(k), day)))
    load = pltpu.make_async_copy(field, own.at[pl.ds(STEP, count)], local_sem)
    load.start()
    waits = {0: 2, **{k: 4 for k in reach[1:]}, PLANES - 1: 3 + RELAYS}
    for spot in range(PLANES):
        at(spot)()(functools.partial(pl.semaphore_wait, barrier, waits.get(spot, 3)))

    def tell(slot, *partners):
        for partner in partners:
            pl.semaphore_signal(ready.at[slot], inc=1, device_id=partner, device_id_type=MESH)

    pl.when(plane != 0)(functools.partial(tell, 0, (west, day)))

    @pl.when(eastmost)
    def _():
        tell(1, (east, day))
        tell(2, *[(level(-k), day) for k in reach[1:]])

    for k in reach:
        at(k)()(functools.partial(tell, 3, (level(-k), day)))

    def remote(source, target, slot, device, sent=None):
        return pltpu.make_async_remote_copy(
            src_ref=source, dst_ref=target, send_sem=send.at[slot if sent is None else sent], recv_sem=recv.at[slot],
            device_id=device, device_id_type=MESH,
        )

    def start(*copies):
        for copy in copies:
            copy.start()

    def arrive(*copies):
        for copy in copies:
            copy.wait_recv()

    def span(group):
        return pl.ds(STEP * group, STEP)

    head_rows = pl.ds(pl.multiple_of(TILE * core, TILE), TILE)
    final = groups - 1
    thin = final - 2
    holders = (0, final, *range(1, REST - 1))

    to_east = remote(field.at[span(final)], own.at[span(0)], 0, (east, day))
    to_west = remote(field.at[span(0)], own.at[span(groups + 1)], 1, (west, day))
    near_all = remote(field, near.at[pl.ds(STEP, count)], 2, (here, near_day))
    near_west = remote(own.at[span(0)], near.at[span(0)], 3, (here, near_day))
    near_east = remote(own.at[span(groups + 1)], near.at[span(groups + 1)], 4, (here, near_day))
    east_head_direct = remote(field.at[span(final), head_rows], heads.at[span(0)], 5, (east, far_day))
    west_head_direct = remote(field.at[span(0), head_rows], heads.at[span(groups + 1)], 6, (west, far_day))
    east_tail_direct = remote(packed.at[final], tails.at[0], 7, (east, far_day))
    west_tail_direct = remote(packed.at[0], tails.at[groups + 1], 8, (west, far_day))
    east_head = remote(heads.at[span(groups)], heads.at[span(0)], 5, (east, day))
    west_head = remote(heads.at[span(1)], heads.at[span(groups + 1)], 6, (west, day))
    east_tail = remote(tails.at[groups], tails.at[0], 7, (east, day))
    west_tail = remote(tails.at[1], tails.at[groups + 1], 8, (west, day))
    spot = 9 + 2 * groups
    cut = [pl.ds(KEPT + SHARE * (k - 1), SHARE) for k in reach]
    kept = pl.ds(0, KEPT)

    turned = spot + RELAYS + 1
    east_part = [remote(apart.at[kept], wrap_rests.at[kept], turned, (east, day))]
    east_part += [remote(apart.at[cut[k - 1]], relayed, spot, (level(k + 1), day), spot + k) for k in reach]
    west_part = [remote(apart.at[kept], wrap_rests.at[kept], turned, (west, day))]
    west_part += [remote(apart.at[cut[k - 1]], relayed, spot, (level(-k - 1), day), spot + k) for k in reach]
    east_pass = [remote(relayed, wrap_rests.at[cut[k - 1]], turned, (level(-k), day), spot) for k in reach]
    west_pass = [remote(relayed, wrap_rests.at[cut[k - 1]], turned, (level(k), day), spot) for k in reach]
    wrap_rest = remote(apart, wrap_rests, turned, (east, day))
    east_wrap = (
        remote(heads.at[span(groups)], wrap_heads, turned + 1, (east, far_day)),
        remote(tails.at[groups], wrap_tails, turned + 2, (east, far_day)),
    )
    west_wrap = (
        remote(heads.at[span(1)], wrap_heads, turned + 1, (west, far_day)),
        remote(tails.at[1], wrap_tails, turned + 2, (west, far_day)),
    )
    sides = tuple(
        remote(source, target, turned + 3 + i, (here, near_day))
        for i, (source, target) in enumerate(((wrap_heads, side_heads), (wrap_tails, side_tails), (wrap_rests, side_rests)))
    )

    def each_plane(eastward, westward, act):
        for k in reach:
            pl.when(plane == k)(functools.partial(act, eastward[k - 1]))
            pl.when(plane == PLANES - 1 - k)(functools.partial(act, westward[k - 1]))

    far_head = [
        remote(
            field.at[span(g), head_rows], last_heads if g == final - 1 else heads.at[span(g + 1)], 9 + g, (here, far_day)
        )
        for g in range(groups)
    ]
    far_tail = [
        remote(
            packed.at[g, pl.ds(0, DENSE)] if g == thin else packed.at[g],
            last_tails if g == final - 1 else tails.at[g + 1, pl.ds(0, DENSE)] if g == thin else tails.at[g + 1],
            9 + groups + g, (here, far_day),
        )
        for g in range(groups)
    ]

    start(far_head[0], far_head[final])

    @pl.when(plane != 0)
    def _():
        start(to_west)

    start(near_all)
    load.wait()

    def rest(lon):
        rows = pl.ds(pl.multiple_of(TILE + TILE * core, TILE), REST)
        return own[lon, rows, :].astype(jnp.float32)

    for i in range(STEP - 1 - REST):
        strayed[i, 0:REST, :] = rest(STEP * (thin + 1) + REST + i)

    def pack(group, _):
        base = STEP * (group + 1)
        spare = rest(base + STEP - 1)
        row = jnp.where(group == 0, 0, jnp.where(group == final, 1, jnp.minimum(group + 1, REST - 1)))
        for j in range(STEP - 1):
            extra = spare[j : j + 1] if j < REST else strayed[j - REST, pl.ds(row, 1), :]
            tile = jnp.concatenate([rest(base + j), extra], axis=0)
            packed[group, TILE * j : TILE * (j + 1), :] = tile.astype(jnp.bfloat16)
        return _

    lax.fori_loop(0, groups, pack, 0)

    ends = (plane == 0) | eastmost
    wrapped = plane // (PLANES - 1)

    @pl.when(ends)
    def _():
        def part(j, _):
            lon = STEP + STEP * final * wrapped + j
            low = own[lon, 0:TILE, :].astype(jnp.float32)
            high = own[lon, TILE:, :].astype(jnp.float32)
            apart[j] = jnp.where(core == 0, high[REST:], low).astype(jnp.bfloat16)
            return _

        lax.fori_loop(0, STEP, part, 0)

    start(far_tail[0], far_tail[final])

    @pl.when(eastmost)
    def _():
        start(east_part[0])

    for g in range(1, final):
        start(far_head[g], far_tail[g])

    @pl.when(plane != PLANES - 1)
    def _():
        pl.semaphore_wait(ready.at[0], 1)
        start(to_east)

    @pl.when(plane == 0)
    def _():
        pl.semaphore_wait(ready.at[1], 1)
        pl.semaphore_wait(ready.at[3], RELAYS)
        tell(4, (west, day))
        start(*west_part, west_head_direct, west_tail_direct)

    @pl.when(eastmost)
    def _():
        pl.semaphore_wait(ready.at[4], 1)
        start(*east_part[1:], east_head_direct, east_tail_direct)

    for k in reach[1:]:
        at(PLANES - 1 - k)()(functools.partial(pl.semaphore_wait, ready.at[2], 1))

    def forward(copy):
        arrive(east_part[1])
        start(copy)

    each_plane(east_pass, west_pass, forward)

    @pl.when(plane != 0)
    def _():
        arrive(to_east)
        start(near_west)

    @pl.when(plane != PLANES - 1)
    def _():
        arrive(to_west)
        start(near_east)

    arrive(far_head[0], far_head[final], far_tail[0], far_tail[final])

    @pl.when(plane != PLANES - 1)
    def _():
        start(east_head, east_tail)

    @pl.when(plane != 0)
    def _():
        start(west_head, west_tail)

    @pl.when(eastmost)
    def _():
        start(*east_wrap)

    @pl.when(plane == 0)
    def _():
        start(*west_wrap)

    @pl.when(ends)
    def _():
        arrive(wrap_rest, *east_wrap)
        start(*sides)

    day_of = lax.broadcasted_iota(jnp.int32, weights.shape[1:], 0)
    place = lax.broadcasted_iota(jnp.int32, weights.shape[1:], 1)

    def window(position, valid=True):
        inside = (jnp.abs(position - day_of) <= DAY_HALF) & valid
        return jnp.where(inside, -1.0, 0.0)

    block = own.shape[1]
    earlier, later = 1 - core, core
    weights[0] = (window(place) + jnp.where(place == day_of, 2.0 * DAY_HALF + 1.0, 0.0)).astype(jnp.bfloat16)
    weights[1] = window(place + block * (earlier - later)).astype(jnp.bfloat16)
    weights[2] = window(place - DAY_HALF * earlier + block * later).astype(jnp.bfloat16)
    weights[3] = window(place - REST * earlier + (block + TILE) * later, place < REST).astype(jnp.bfloat16)
    which = place // TILE
    stray = (place % TILE == REST) & (which < REST)
    weights[4] = window(which - REST * earlier + (block + TILE) * later, stray).astype(jnp.bfloat16)

    @pl.when(ends)
    def _():
        for i, (shift, which_core, center) in enumerate(((0, core, 1.0), (block * (earlier - later), 1 - core, 0.0))):
            base = TILE + TILE * which_core + shift
            spots = (
                (place + base - TILE, True), (place + base, place < REST), (which + base, stray),
                (place + DAY_HALF * (1 - which_core) + shift, True),
            )
            for n, (position, valid) in enumerate(spots):
                peak = jnp.where((position == day_of) & valid, center * (2.0 * DAY_HALF + 1.0), 0.0)
                weights[5 + 4 * i + n] = (window(position, valid) + peak).astype(jnp.bfloat16)

    dot, strip = functools.partial(product, weights), functools.partial(strips, weights)

    def term(group, _):
        group_terms(group, weights, own, near, heads, tails, terms)
        return _

    def wrap_term(group):
        for j in range(STEP):
            lon = STEP * group + j
            total = dot(2, TILE, heads[lon]) + strip(3, tails.at[group], j)
            total += dot(5, TILE, wrap_heads[j]) + strip(6, wrap_tails, j) + dot(8, TILE, wrap_rests[j])
            total += dot(9, TILE, side_heads[j]) + strip(10, side_tails, j) + dot(12, TILE, side_rests[j])
            terms[lon] = total

    arrive(near_all)
    lax.fori_loop(0, 2, lambda i, c: term(1 + final * i, c), 0)
    arrive(far_head[1], far_tail[1])
    term(2, 0)
    total = opening(terms, 1)
    corner = final // 2 + 1
    for g in range(2, final):
        if g < final - 1:
            arrive(far_head[g], far_tail[g])
            if g == thin:
                for i in range(STEP - 1 - REST):
                    place_in = pl.ds(TILE * (REST + i), TILE)
                    for n, holder in enumerate(holders):
                        moved[i, TILE * n : TILE * (n + 1), :] = tails[holder + 1, place_in, :]
                group_terms(g + 1, weights, own, near, heads, tails, terms, moved)
            else:
                term(g + 1, 0)
        else:
            for lon in range(STEP * (g + 1), STEP * (g + 2)):
                terms[lon] = dot(0, block, own[lon]) + dot(1, block, near[lon])
            arrive(far_head[g], far_tail[g])
        if g - 1 < groups - LATE:
            total = results(terms, done, g - 1, 0, total)
        if g == corner:
            arrive(east_head, west_head, east_tail, west_tail)

            @pl.when(plane != 0)
            def _():
                arrive(near_west)
                term(0, 0)

            @pl.when(plane != PLANES - 1)
            def _():
                arrive(near_east)
                term(groups + 1, 0)

            @pl.when(ends)
            def _():
                arrive(*sides)
                wrap_term((groups + 1) * wrapped)

            results(terms, done, 0, 0, opening(terms, 0))

    def finish(*copies):
        for copy in copies:
            copy.wait_send()

    each_plane(east_pass, west_pass, finish)

    @pl.when(eastmost)
    def _():
        finish(*east_part, *east_wrap)

    @pl.when(plane != PLANES - 1)
    def _():
        finish(to_east, near_east)

    @pl.when(plane == 0)
    def _():
        finish(*west_part, *west_wrap)

    @pl.when(plane != 0)
    def _():
        finish(to_west, near_west)

    @pl.when(ends)
    def _():
        finish(*sides)

    for copy in (near_all, east_head, west_head, east_tail, west_tail):
        copy.wait_send()
    for copy in far_head + far_tail:
        copy.wait_send()


def solution(mesh):
    lons, days = mesh.shape["lon"], mesh.shape["day"]

    def local(field):
        rows, count, columns = field.shape
        groups = count // STEP
        wide = count + 2 * STEP
        slots = 16 + 2 * groups + RELAYS
        wrap_edges = [(STEP, TILE, columns), (PACKED, columns), (STEP, TILE, columns)]
        vmem = pl.BlockSpec(memory_space=pltpu.VMEM)
        gathered = pl.pallas_call(
            functools.partial(kernel, lons, days),
            out_shape=(
                pltpu.VMEM((count - LATE * STEP, rows, columns), jnp.float32),
                pltpu.VMEM((wide, rows, columns), jnp.float32),
                pltpu.VMEM((STEP, TILE, columns), jnp.bfloat16),
                pltpu.VMEM((PACKED, columns), jnp.bfloat16),
                pltpu.VMEM((13, rows, PACKED), jnp.bfloat16),
            ),
            in_specs=[pl.BlockSpec(memory_space=pltpu.HBM)],
            out_specs=(vmem,) * 5,
            scratch_shapes=[
                pltpu.VMEM((wide, rows, columns), jnp.bfloat16),
                pltpu.VMEM((wide, rows, columns), jnp.bfloat16),
                pltpu.VMEM((wide, TILE, columns), jnp.bfloat16),
                pltpu.VMEM((groups + 2, PACKED, columns), jnp.bfloat16),
                pltpu.VMEM((groups, PACKED, columns), jnp.bfloat16),
                pltpu.VMEM((STEP - 1 - REST, TILE, columns), jnp.float32),
                pltpu.VMEM((STEP - 1 - REST, DENSE, columns), jnp.bfloat16),
                pltpu.VMEM((SHARE, TILE, columns), jnp.bfloat16),
                pltpu.SemaphoreType.REGULAR((5,)),
                pltpu.VMEM((STEP, TILE, columns), jnp.bfloat16),
                *[pltpu.VMEM(edge, jnp.bfloat16) for edge in 2 * wrap_edges],
                pltpu.SemaphoreType.DMA,
                pltpu.SemaphoreType.DMA((slots,)),
                pltpu.SemaphoreType.DMA((slots,)),
            ],
            compiler_params=pltpu.CompilerParams(
                collective_id=0, has_side_effects=True, vmem_limit_bytes=40 * 1024 * 1024
            ),
            name="anomaly",
        )(jnp.transpose(field, (1, 0, 2)))
        result = pl.pallas_call(
            finishing,
            out_shape=jax.ShapeDtypeStruct((count, rows, columns), jnp.float32),
            in_specs=[vmem] * 5,
            out_specs=pl.BlockSpec(memory_space=pl.ANY),
            scratch_shapes=[
                pltpu.VMEM((STEP, rows, columns), jnp.float32),
                pltpu.VMEM((LATE * STEP, rows, columns), jnp.float32),
                pltpu.SemaphoreType.DMA((groups,)),
            ],
            compiler_params=pltpu.CompilerParams(vmem_limit_bytes=16 * 1024 * 1024),
            name="finishing",
        )(*gathered)
        return jnp.transpose(result, (1, 0, 2))

    return jax.shard_map(
        local, mesh=mesh, in_specs=(P("day", "lon", None),), out_specs=P("day", "lon", None), check_vma=False
    )
```

```python
import functools

import jax
import jax.numpy as jnp
from jax import lax
from jax.experimental import pallas as pl
from jax.experimental.pallas import tpu as pltpu
from jax.sharding import PartitionSpec as P

DAY_HALF = 15
LON_HALF = 10
PLANES = 8
TILE = 8
REST = DAY_HALF - TILE
STEP = LON_HALF
PACKED = (STEP - 1) * TILE
DENSE = REST * TILE
SCALE = 1.0 / ((2 * DAY_HALF + 1) * (2 * LON_HALF + 1))
RELAYS = 3
LATE = 3
SHARE = 3
KEPT = STEP - RELAYS * SHARE
MESH = pl.DeviceIdType.MESH


def product(weights, which, columns, values):
    return jnp.dot(weights[which, :, 0:columns], values, preferred_element_type=jnp.float32)


def strips(weights, first, tail, j):
    if j < STEP - 1:
        return product(weights, first, TILE, tail[TILE * j : TILE * (j + 1), :])
    return product(weights, first + 1, PACKED, tail[...])


def group_terms(group, weights, own, near, heads, tails, terms, moved=None):
    block = own.shape[1]
    for j in range(STEP):
        lon = STEP * group + j
        total = product(weights, 0, block, own[lon]) + product(weights, 1, block, near[lon])
        total += product(weights, 2, TILE, heads[lon])
        if moved is None or j < REST:
            total += strips(weights, 3, tails.at[group], j)
        else:
            rows = tails[group, 0:DENSE, :] if j == STEP - 1 else moved[j - REST]
            total += product(weights, 4, DENSE, rows)
        terms[lon] = total


def results(terms, target, group, first, total):
    def result(lon, total):
        total = total + terms[lon + 2 * STEP]
        target[lon - STEP * first] = total * SCALE
        return total - terms[lon]

    return lax.fori_loop(STEP * group, STEP * (group + 1), result, total)


def opening(terms, group):
    zero = jnp.zeros(terms.shape[1:], jnp.float32)
    return lax.fori_loop(STEP * group, STEP * (group + 2), lambda lon, total: total + terms[lon], zero)


def finishing(done, terms, heads, tails, weights, out, fresh, late, sems):
    early = done.shape[0] // STEP

    def put(source, group, first):
        return pltpu.make_async_copy(
            source.at[pl.ds(STEP * (group - first), STEP)], out.at[pl.ds(STEP * group, STEP)], sems.at[group]
        )

    copies = [put(done, group, 0) for group in range(early)]
    for copy in copies:
        copy.start()
    zero = jnp.zeros(terms.shape[1:], jnp.float32)
    total = lax.fori_loop(STEP * early, STEP * (early + 2), lambda lon, total: total + terms[lon], zero)
    for j in range(STEP):
        far = product(weights, 2, TILE, heads[j]) + strips(weights, 3, tails, j)
        fresh[j] = terms[STEP * (early + 2) + j] + far
    for group in range(early, early + LATE):

        def result(i, total):
            lon = STEP * group + i
            total = total + (fresh[i] if group == early else terms[lon + 2 * STEP])
            late[lon - STEP * early] = total * SCALE
            return total - (fresh[i] if group == early + 2 else terms[lon])

        total = lax.fori_loop(0, STEP, result, total)
        copies.append(put(late, group, early))
        copies[-1].start()
    for copy in copies:
        copy.wait()


def kernel(
    lons, days, field, done, terms, last_heads, last_tails, weights, own, near, heads, tails, packed, strayed, moved, relayed, ready,
    apart, wrap_heads, wrap_tails, wrap_rests, side_heads, side_tails, side_rests, local_sem, send, recv,
):
    count = field.shape[0]
    columns = field.shape[2]
    groups = count // STEP
    here = lax.axis_index("lon")
    day = lax.axis_index("day")
    core = lax.rem(day, 2)
    turn = 2 * core - 1
    far_day = lax.rem(day + turn + days, days)
    near_day = lax.rem(day - turn + days, days)
    east = lax.rem(here + 1, lons)
    west = lax.rem(here + lons - 1, lons)
    plane = lax.rem(here, PLANES)

    barrier = pltpu.get_barrier_semaphore()

    def level(offset):
        return lax.rem(here + offset + lons, lons)

    def greet(*partners):
        for partner in partners:
            pl.semaphore_signal(barrier, inc=1, device_id=partner, device_id_type=MESH)

    reach = range(1, RELAYS + 1)
    eastmost = plane == PLANES - 1

    def at(spot):
        return functools.partial(pl.when, plane == spot)

    greet((here, far_day), (here, near_day))
    pl.when(plane != PLANES - 1)(functools.partial(greet, (east, day)))
    at(0)()(
        functools.partial(
            greet, (west, day), *[(level(k), day) for k in reach[1:]]
        )
    )
    for k in reach[1:]:
        at(PLANES - 1 - k)()(functools.partial(greet, (level(k), day)))
    load = pltpu.make_async_copy(field, own.at[pl.ds(STEP, count)], local_sem)
    load.start()
    waits = {0: 2, **{k: 4 for k in reach[1:]}, PLANES - 1: 3 + RELAYS}
    for spot in range(PLANES):
        at(spot)()(functools.partial(pl.semaphore_wait, barrier, waits.get(spot, 3)))

    def tell(slot, *partners):
        for partner in partners:
            pl.semaphore_signal(ready.at[slot], inc=1, device_id=partner, device_id_type=MESH)

    pl.when(plane != 0)(functools.partial(tell, 0, (west, day)))

    @pl.when(eastmost)
    def _():
        tell(1, (east, day))
        tell(2, *[(level(-k), day) for k in reach[1:]])

    for k in reach:
        at(k)()(functools.partial(tell, 3, (level(-k), day)))

    def remote(source, target, slot, device, sent=None):
        return pltpu.make_async_remote_copy(
            src_ref=source, dst_ref=target, send_sem=send.at[slot if sent is None else sent], recv_sem=recv.at[slot],
            device_id=device, device_id_type=MESH,
        )

    def start(*copies):
        for copy in copies:
            copy.start()

    def arrive(*copies):
        for copy in copies:
            copy.wait_recv()

    def span(group):
        return pl.ds(STEP * group, STEP)

    head_rows = pl.ds(pl.multiple_of(TILE * core, TILE), TILE)
    final = groups - 1
    thin = final - 2
    holders = (0, final, *range(1, REST - 1))

    to_east = remote(field.at[span(final)], own.at[span(0)], 0, (east, day))
    to_west = remote(field.at[span(0)], own.at[span(groups + 1)], 1, (west, day))
    near_all = remote(field, near.at[pl.ds(STEP, count)], 2, (here, near_day))
    near_west = remote(own.at[span(0)], near.at[span(0)], 3, (here, near_day))
    near_east = remote(own.at[span(groups + 1)], near.at[span(groups + 1)], 4, (here, near_day))
    east_head_direct = remote(field.at[span(final), head_rows], heads.at[span(0)], 5, (east, far_day))
    west_head_direct = remote(field.at[span(0), head_rows], heads.at[span(groups + 1)], 6, (west, far_day))
    east_tail_direct = remote(packed.at[final], tails.at[0], 7, (east, far_day))
    west_tail_direct = remote(packed.at[0], tails.at[groups + 1], 8, (west, far_day))
    east_head = remote(heads.at[span(groups)], heads.at[span(0)], 5, (east, day))
    west_head = remote(heads.at[span(1)], heads.at[span(groups + 1)], 6, (west, day))
    east_tail = remote(tails.at[groups], tails.at[0], 7, (east, day))
    west_tail = remote(tails.at[1], tails.at[groups + 1], 8, (west, day))
    spot = 9 + 2 * groups
    cut = [pl.ds(KEPT + SHARE * (k - 1), SHARE) for k in reach]
    kept = pl.ds(0, KEPT)

    turned = spot + RELAYS + 1
    east_part = [remote(apart.at[kept], wrap_rests.at[kept], turned, (east, day))]
    east_part += [remote(apart.at[cut[k - 1]], relayed, spot, (level(k + 1), day), spot + k) for k in reach]
    west_part = [remote(apart.at[kept], wrap_rests.at[kept], turned, (west, day))]
    west_part += [remote(apart.at[cut[k - 1]], relayed, spot, (level(-k - 1), day), spot + k) for k in reach]
    east_pass = [remote(relayed, wrap_rests.at[cut[k - 1]], turned, (level(-k), day), spot) for k in reach]
    west_pass = [remote(relayed, wrap_rests.at[cut[k - 1]], turned, (level(k), day), spot) for k in reach]
    wrap_rest = remote(apart, wrap_rests, turned, (east, day))
    east_wrap = (
        remote(heads.at[span(groups)], wrap_heads, turned + 1, (east, far_day)),
        remote(tails.at[groups], wrap_tails, turned + 2, (east, far_day)),
    )
    west_wrap = (
        remote(heads.at[span(1)], wrap_heads, turned + 1, (west, far_day)),
        remote(tails.at[1], wrap_tails, turned + 2, (west, far_day)),
    )
    sides = tuple(
        remote(source, target, turned + 3 + i, (here, near_day))
        for i, (source, target) in enumerate(((wrap_heads, side_heads), (wrap_tails, side_tails), (wrap_rests, side_rests)))
    )

    def each_plane(eastward, westward, act):
        for k in reach:
            pl.when(plane == k)(functools.partial(act, eastward[k - 1]))
            pl.when(plane == PLANES - 1 - k)(functools.partial(act, westward[k - 1]))

    far_head = [
        remote(
            field.at[span(g), head_rows], last_heads if g == final - 1 else heads.at[span(g + 1)], 9 + g, (here, far_day)
        )
        for g in range(groups)
    ]
    far_tail = [
        remote(
            packed.at[g, pl.ds(0, DENSE)] if g == thin else packed.at[g],
            last_tails if g == final - 1 else tails.at[g + 1, pl.ds(0, DENSE)] if g == thin else tails.at[g + 1],
            9 + groups + g, (here, far_day),
        )
        for g in range(groups)
    ]

    start(far_head[0], far_head[final])

    @pl.when(plane != 0)
    def _():
        start(to_west)

    start(near_all)
    load.wait()

    def rest(lon):
        rows = pl.ds(pl.multiple_of(TILE + TILE * core, TILE), REST)
        return own[lon, rows, :].astype(jnp.float32)

    for i in range(STEP - 1 - REST):
        strayed[i, 0:REST, :] = rest(STEP * (thin + 1) + REST + i)

    def pack(turn_of, _):
        group = lax.rem(turn_of + final, groups)
        base = STEP * (group + 1)
        spare = rest(base + STEP - 1)
        row = jnp.where(group == 0, 0, jnp.where(group == final, 1, jnp.minimum(group + 1, REST - 1)))
        for j in range(STEP - 1):
            extra = spare[j : j + 1] if j < REST else strayed[j - REST, pl.ds(row, 1), :]
            tile = jnp.concatenate([rest(base + j), extra], axis=0)
            packed[group, TILE * j : TILE * (j + 1), :] = tile.astype(jnp.bfloat16)
        return _

    lax.fori_loop(0, groups, pack, 0)

    ends = (plane == 0) | eastmost
    wrapped = plane // (PLANES - 1)

    @pl.when(ends)
    def _():
        def part(j, _):
            lon = STEP + STEP * final * wrapped + j
            low = own[lon, 0:TILE, :].astype(jnp.float32)
            high = own[lon, TILE:, :].astype(jnp.float32)
            apart[j] = jnp.where(core == 0, high[REST:], low).astype(jnp.bfloat16)
            return _

        lax.fori_loop(0, STEP, part, 0)

    start(far_tail[0], far_tail[final])

    for g in range(1, final):
        start(far_head[g], far_tail[g])

    @pl.when(eastmost)
    def _():
        start(east_part[0])

    @pl.when(plane != PLANES - 1)
    def _():
        pl.semaphore_wait(ready.at[0], 1)
        start(to_east)

    @pl.when(plane == 0)
    def _():
        pl.semaphore_wait(ready.at[1], 1)
        pl.semaphore_wait(ready.at[3], RELAYS)
        tell(4, (west, day))
        start(*west_part, west_head_direct, west_tail_direct)

    @pl.when(eastmost)
    def _():
        pl.semaphore_wait(ready.at[4], 1)
        start(*east_part[1:], east_head_direct, east_tail_direct)

    for k in reach[1:]:
        at(PLANES - 1 - k)()(functools.partial(pl.semaphore_wait, ready.at[2], 1))

    def forward(copy):
        arrive(east_part[1])
        start(copy)

    each_plane(east_pass, west_pass, forward)

    @pl.when(plane != 0)
    def _():
        arrive(to_east)
        start(near_west)

    @pl.when(plane != PLANES - 1)
    def _():
        arrive(to_west)
        start(near_east)

    arrive(far_head[0], far_head[final], far_tail[0], far_tail[final])

    @pl.when(plane != PLANES - 1)
    def _():
        start(east_head, east_tail)

    @pl.when(plane != 0)
    def _():
        start(west_head, west_tail)

    @pl.when(eastmost)
    def _():
        start(*east_wrap)

    @pl.when(plane == 0)
    def _():
        start(*west_wrap)

    @pl.when(ends)
    def _():
        arrive(wrap_rest, *east_wrap)
        start(*sides)

    day_of = lax.broadcasted_iota(jnp.int32, weights.shape[1:], 0)
    place = lax.broadcasted_iota(jnp.int32, weights.shape[1:], 1)

    def window(position, valid=True):
        inside = (jnp.abs(position - day_of) <= DAY_HALF) & valid
        return jnp.where(inside, -1.0, 0.0)

    block = own.shape[1]
    earlier, later = 1 - core, core
    weights[0] = (window(place) + jnp.where(place == day_of, 2.0 * DAY_HALF + 1.0, 0.0)).astype(jnp.bfloat16)
    weights[1] = window(place + block * (earlier - later)).astype(jnp.bfloat16)
    weights[2] = window(place - DAY_HALF * earlier + block * later).astype(jnp.bfloat16)
    weights[3] = window(place - REST * earlier + (block + TILE) * later, place < REST).astype(jnp.bfloat16)
    which = place // TILE
    stray = (place % TILE == REST) & (which < REST)
    weights[4] = window(which - REST * earlier + (block + TILE) * later, stray).astype(jnp.bfloat16)

    @pl.when(ends)
    def _():
        for i, (shift, which_core, center) in enumerate(((0, core, 1.0), (block * (earlier - later), 1 - core, 0.0))):
            base = TILE + TILE * which_core + shift
            spots = (
                (place + base - TILE, True), (place + base, place < REST), (which + base, stray),
                (place + DAY_HALF * (1 - which_core) + shift, True),
            )
            for n, (position, valid) in enumerate(spots):
                peak = jnp.where((position == day_of) & valid, center * (2.0 * DAY_HALF + 1.0), 0.0)
                weights[5 + 4 * i + n] = (window(position, valid) + peak).astype(jnp.bfloat16)

    dot, strip = functools.partial(product, weights), functools.partial(strips, weights)

    def term(group, _):
        group_terms(group, weights, own, near, heads, tails, terms)
        return _

    def wrap_term(group):
        for j in range(STEP):
            lon = STEP * group + j
            total = dot(2, TILE, heads[lon]) + strip(3, tails.at[group], j)
            total += dot(5, TILE, wrap_heads[j]) + strip(6, wrap_tails, j) + dot(8, TILE, wrap_rests[j])
            total += dot(9, TILE, side_heads[j]) + strip(10, side_tails, j) + dot(12, TILE, side_rests[j])
            terms[lon] = total

    arrive(near_all)
    lax.fori_loop(0, 2, lambda i, c: term(1 + final * i, c), 0)
    arrive(far_head[1], far_tail[1])
    term(2, 0)
    total = opening(terms, 1)
    corner = final // 2 + 1
    for g in range(2, final):
        if g < final - 1:
            arrive(far_head[g], far_tail[g])
            if g == thin:
                for i in range(STEP - 1 - REST):
                    place_in = pl.ds(TILE * (REST + i), TILE)
                    for n, holder in enumerate(holders):
                        moved[i, TILE * n : TILE * (n + 1), :] = tails[holder + 1, place_in, :]
                group_terms(g + 1, weights, own, near, heads, tails, terms, moved)
            else:
                term(g + 1, 0)
        else:
            for lon in range(STEP * (g + 1), STEP * (g + 2)):
                terms[lon] = dot(0, block, own[lon]) + dot(1, block, near[lon])
            arrive(far_head[g], far_tail[g])
        if g - 1 < groups - LATE:
            total = results(terms, done, g - 1, 0, total)
        if g == corner:
            arrive(east_head, west_head, east_tail, west_tail)

            @pl.when(plane != 0)
            def _():
                arrive(near_west)
                term(0, 0)

            @pl.when(plane != PLANES - 1)
            def _():
                arrive(near_east)
                term(groups + 1, 0)

            @pl.when(ends)
            def _():
                arrive(*sides)
                wrap_term((groups + 1) * wrapped)

            results(terms, done, 0, 0, opening(terms, 0))

    def finish(*copies):
        for copy in copies:
            copy.wait_send()

    each_plane(east_pass, west_pass, finish)

    @pl.when(eastmost)
    def _():
        finish(*east_part, *east_wrap)

    @pl.when(plane != PLANES - 1)
    def _():
        finish(to_east, near_east)

    @pl.when(plane == 0)
    def _():
        finish(*west_part, *west_wrap)

    @pl.when(plane != 0)
    def _():
        finish(to_west, near_west)

    @pl.when(ends)
    def _():
        finish(*sides)

    for copy in (near_all, east_head, west_head, east_tail, west_tail):
        copy.wait_send()
    for copy in far_head + far_tail:
        copy.wait_send()


def solution(mesh):
    lons, days = mesh.shape["lon"], mesh.shape["day"]

    def local(field):
        rows, count, columns = field.shape
        groups = count // STEP
        wide = count + 2 * STEP
        slots = 16 + 2 * groups + RELAYS
        wrap_edges = [(STEP, TILE, columns), (PACKED, columns), (STEP, TILE, columns)]
        vmem = pl.BlockSpec(memory_space=pltpu.VMEM)
        gathered = pl.pallas_call(
            functools.partial(kernel, lons, days),
            out_shape=(
                pltpu.VMEM((count - LATE * STEP, rows, columns), jnp.float32),
                pltpu.VMEM((wide, rows, columns), jnp.float32),
                pltpu.VMEM((STEP, TILE, columns), jnp.bfloat16),
                pltpu.VMEM((PACKED, columns), jnp.bfloat16),
                pltpu.VMEM((13, rows, PACKED), jnp.bfloat16),
            ),
            in_specs=[pl.BlockSpec(memory_space=pltpu.HBM)],
            out_specs=(vmem,) * 5,
            scratch_shapes=[
                pltpu.VMEM((wide, rows, columns), jnp.bfloat16),
                pltpu.VMEM((wide, rows, columns), jnp.bfloat16),
                pltpu.VMEM((wide, TILE, columns), jnp.bfloat16),
                pltpu.VMEM((groups + 2, PACKED, columns), jnp.bfloat16),
                pltpu.VMEM((groups, PACKED, columns), jnp.bfloat16),
                pltpu.VMEM((STEP - 1 - REST, TILE, columns), jnp.float32),
                pltpu.VMEM((STEP - 1 - REST, DENSE, columns), jnp.bfloat16),
                pltpu.VMEM((SHARE, TILE, columns), jnp.bfloat16),
                pltpu.SemaphoreType.REGULAR((5,)),
                pltpu.VMEM((STEP, TILE, columns), jnp.bfloat16),
                *[pltpu.VMEM(edge, jnp.bfloat16) for edge in 2 * wrap_edges],
                pltpu.SemaphoreType.DMA,
                pltpu.SemaphoreType.DMA((slots,)),
                pltpu.SemaphoreType.DMA((slots,)),
            ],
            compiler_params=pltpu.CompilerParams(
                collective_id=0, has_side_effects=True, vmem_limit_bytes=40 * 1024 * 1024
            ),
            name="anomaly",
        )(jnp.transpose(field, (1, 0, 2)))
        result = pl.pallas_call(
            finishing,
            out_shape=jax.ShapeDtypeStruct((count, rows, columns), jnp.float32),
            in_specs=[vmem] * 5,
            out_specs=pl.BlockSpec(memory_space=pl.ANY),
            scratch_shapes=[
                pltpu.VMEM((STEP, rows, columns), jnp.float32),
                pltpu.VMEM((LATE * STEP, rows, columns), jnp.float32),
                pltpu.SemaphoreType.DMA((groups,)),
            ],
            compiler_params=pltpu.CompilerParams(vmem_limit_bytes=16 * 1024 * 1024),
            name="finishing",
        )(*gathered)
        return jnp.transpose(result, (1, 0, 2))

    return jax.shard_map(
        local, mesh=mesh, in_specs=(P("day", "lon", None),), out_specs=P("day", "lon", None), check_vma=False
    )
```
